128 devices in a mesh: vol: 16 (over y, z), pix: 8 (over x, core).
Axes of the slice: x: 4, y: 4, z: 4, core: 2. Of those that a mesh axis runs over, the one named last changes fastest.
Arguments:
- kernel: bfloat16 [2097152, 128], P(('vol', 'pix')), may hold values from 0 to 0.25
- pressure: bfloat16 [2097152], P(('vol', 'pix')), may hold values from 0.049804688 to 2
- velocity: bfloat16 [2097152], P(('vol', 'pix')), may hold values from -4 to 4
- entry_slot: int32 [128, 16384], P(('vol', 'pix')), may hold values from 0 to 1023, never falling along the last dimension, each value on 1 to 32 neighbouring positions
- slot_tile: int32 [128, 1024], P(('vol', 'pix')), may hold values from 0 to 32767, as said below
- tile_owner: int32 [32768], replicated, may hold values from 0 to 7, as said below
Outputs:
- owned_tiles: float32 [65536, 256], P(('vol', 'pix'))
- shell_map: float32 [32768, 256], P('vol')
The draws below stay inside these ranges and needn't reach their ends.
Inputs may be any that keep to these rules, and one draw needn't show every extreme that they name: `entry_slot`: for each device the slot numbers never fall along its 16384 crossings; every slot has at least one crossing and at most 32. `tile_owner`: within every block of 2048 consecutive tiles each pix index owns 256 // 2 to 512 tiles, and one owner of each block owns exactly 512. `slot_tile`: the 1024 tiles of one device are distinct; at most 16 of them belong to any one owning device (vol index t // 2048, pix index tile_owner[t]), and one owning device gets exactly 16 from every device.
All inputs are finite; a program needn't handle non-finite values.
Results may differ from the reference program's by a relative error of at most 0.0003.
Values sent between devices are 32-bit elements; how exact they have to be, the bound alone decides.
A program may use at most 64 MiB of HBM per device.

```python
import math
import jax
import jax.numpy as jnp
import numpy as np
from jax import lax

PIX_TILE = 128
CHANNELS = 2
ENTRIES = 16384
SLOTS = 1024
TILE_DEV = 256
TILE_V = 2048
TILES = 32768
OWN_MAX = 512
CAP = 16
N_VOL = 16
N_PIX = 8
DEVICES = 128


def ownership(key):
    groups = TILE_V // TILE_DEV
    vol_count = TILES // TILE_V
    least_owned = TILE_DEV // 2
    most_owned = 2 * TILE_DEV
    remainder = TILE_V - most_owned - (groups - 1) * least_owned
    labels = jnp.arange(groups, dtype=jnp.int32)

    def one_block(block_key):
        busiest_key, pool_key, mix_key = jax.random.split(block_key, 3)
        busiest = jax.random.randint(busiest_key, (), 0, groups, dtype=jnp.int32)
        baseline = jnp.repeat(labels, least_owned)
        extra_top = jnp.full((most_owned - least_owned,), 1, jnp.int32) * busiest
        token_pool = jax.random.permutation(pool_key, jnp.repeat(labels, most_owned - least_owned))
        ordering = jnp.argsort((token_pool == busiest).astype(jnp.int32), stable=True)
        chosen = token_pool[ordering][:remainder]
        block_owner = jnp.concatenate([baseline, extra_top, chosen]).astype(jnp.int32)
        return (jax.random.permutation(mix_key, block_owner), busiest)
    owners, busiest_overall = jax.vmap(one_block)(jax.random.split(key, vol_count))
    heavy_vol = jax.random.randint(jax.random.fold_in(key, 7), (), 0, vol_count, dtype=jnp.int32)
    heavy_device = heavy_vol * groups + busiest_overall[heavy_vol]
    return (owners.astype(jnp.int32), heavy_device.astype(jnp.int32))


def draw_tile_owner(key, part):
    owners, heavy_device = ownership(jax.random.fold_in(key, 101))
    return owners.reshape(TILES)


def draw_slot_tile(key, part):
    owners, heavy_device = ownership(jax.random.fold_in(key, 101))
    groups = TILE_V // TILE_DEV
    vol_count = TILES // TILE_V
    device_count = vol_count * groups
    flat_owner = owners.reshape(TILES)
    holder = jnp.arange(TILES, dtype=jnp.int32) // TILE_V * groups + flat_owner
    held_count = jax.ops.segment_sum(jnp.ones((TILES,), jnp.int32), holder, num_segments=device_count)
    first_row = (jnp.cumsum(held_count, dtype=jnp.int32) - held_count).astype(jnp.int32)
    labels = jnp.arange(device_count, dtype=jnp.int32)

    def one_device(device_key):
        pool_key, ranking_random_key, mix_key = jax.random.split(device_key, 3)
        token_pool = jax.random.permutation(pool_key, jnp.repeat(labels, CAP))
        ordering = jnp.argsort((token_pool == heavy_device).astype(jnp.int32), stable=True)
        chosen = token_pool[ordering][:SLOTS - CAP]
        wanted = jax.ops.segment_sum(jnp.ones((SLOTS - CAP,), jnp.int32), chosen, num_segments=device_count)
        wanted = wanted + CAP * (labels == heavy_device).astype(jnp.int32)
        shuffle = jax.random.permutation(ranking_random_key, TILES).astype(jnp.int32)
        grouped = jnp.argsort(holder * TILES + shuffle, stable=True).astype(jnp.int32)
        position = jnp.arange(TILES, dtype=jnp.int32) - first_row[holder[grouped]]
        selected = position < wanted[holder[grouped]]
        positions = jnp.nonzero(selected, size=SLOTS)[0]
        tile_ids = grouped[positions].astype(jnp.int32)
        return jax.random.permutation(mix_key, tile_ids)
    device_keys = jax.random.split(jax.random.fold_in(key, 202), device_count)
    return jax.vmap(one_device)(device_keys).astype(jnp.int32)


def levels(rng, dims, cuts, low, high):
    def one(axis_at, blocks):
        heights = jax.random.uniform(jax.random.fold_in(jax.random.fold_in(rng, 6), axis_at), (blocks,), jnp.float32, low / len(cuts), high / len(cuts))
        return jnp.repeat(jnp.exp(heights), dims[axis_at] // blocks).reshape((-1,) + (1,) * (len(dims) - axis_at - 1))

    factor_of = one(*cuts[0])
    for cut in cuts[1:]:
        factor_of = factor_of * one(*cut)
    return factor_of


def profile(number_of, total, limit, skew):
    loads = [(1 << 20) // math.isqrt(rank ** skew) + 1 for rank in range(2, number_of + 1)]
    spare, counts = total - limit - (number_of - 1), [1] * (number_of - 1)
    while spare > 0:
        candidates = [i for i in range(number_of - 1) if counts[i] < limit]
        pool, left = sum([loads[i] for i in candidates]), spare
        for i in candidates:
            more = min(limit - counts[i], max(1, left * loads[i] // pool), spare)
            counts[i] = counts[i] + more
            spare = spare - more
    return np.array([limit] + counts)


def ragged(stream_key, number_of, total, limit, slope):
    if number_of == 2:
        one = jax.random.randint(stream_key, (), max(1, total - limit), min(limit, total - 1) + 1)
        return jnp.stack([one, total - one])
    tallies = jnp.asarray(profile(number_of, total, limit, slope), jnp.int32)
    twos = (number_of - 1) // 2
    donor, receiver = tallies[1:1 + 2 * twos:2], tallies[2:2 + 2 * twos:2]
    margin = jnp.minimum(donor - 1, limit - receiver)
    passed = jax.random.randint(jax.random.fold_in(stream_key, 1), (twos,), 0, 1 << 20) % (margin + 1)
    tallies = tallies.at[1:1 + 2 * twos:2].set(donor - passed).at[2:2 + 2 * twos:2].set(receiver + passed)
    return tallies[jax.random.permutation(jax.random.fold_in(stream_key, 2), number_of)]


def normal_values(rng, shape, spread, reach, shards=(), kind=jnp.bfloat16):
    loudness = levels(rng, shape, shards, -0.22, 0.18) if shards else 1.0
    values = jax.random.normal(rng, shape, jnp.float32) * spread * loudness
    return jnp.minimum(jnp.maximum(values, -reach), reach).astype(kind)


def setup_inputs(seed: int = 0) -> dict:
    splits = jax.random.split(jax.random.key(seed), 7)
    return {
        "kernel": jnp.clip(0.25 * jax.random.uniform(splits[0], (DEVICES * ENTRIES, PIX_TILE), jnp.float32) ** levels(splits[0], (DEVICES * ENTRIES, PIX_TILE), ((0, 128),), -0.2, 0.2), 0.0, 0.25).astype(jnp.bfloat16),
        "pressure": jnp.clip(jnp.exp(math.log(2.0) - 3.6927934 * jax.random.uniform(splits[1], (DEVICES * ENTRIES,), jnp.float32) ** levels(splits[1], (DEVICES * ENTRIES,), ((0, 128),), -0.2, 0.2)), 0.049804688, 2.0).astype(jnp.bfloat16),
        "velocity": normal_values(splits[2], (DEVICES * ENTRIES,), 1.0, 4.0, ((0, 128),)),
        "entry_slot": jax.vmap(lambda own: jnp.searchsorted(jnp.cumsum(ragged(own, SLOTS, ENTRIES, 2 * ENTRIES // SLOTS, 1)), jnp.arange(ENTRIES), side="right"))(jax.random.split(splits[3], DEVICES)).reshape((DEVICES, ENTRIES)).astype(jnp.int32),
        "slot_tile": draw_slot_tile(jax.random.fold_in(splits[6], 71), 0),
        "tile_owner": draw_tile_owner(jax.random.fold_in(splits[6], 71), 0),
    }


def reference(kernel, pressure, velocity, entry_slot, slot_tile, tile_owner):
    kernel_weights = kernel.reshape(DEVICES, ENTRIES, PIX_TILE)
    amplitude = jnp.stack([pressure, velocity], axis=-1).reshape(DEVICES, ENTRIES, CHANNELS)

    def accumulate(running, inputs):
        device_kernel, device_amplitude, device_slot, device_tile = inputs
        pixel_products = device_amplitude.astype(jnp.float32)[:, :, None] * device_kernel.astype(jnp.float32)[:, None, :]
        partial_value = jax.ops.segment_sum(pixel_products.reshape(ENTRIES, CHANNELS * PIX_TILE), device_slot, num_segments=SLOTS)
        return running.at[device_tile].add(partial_value), None

    start_value = jnp.zeros((TILES, CHANNELS * PIX_TILE), jnp.float32)
    shell_map, unused = lax.scan(accumulate, start_value, (kernel_weights, amplitude, entry_slot, slot_tile))
    owners = tile_owner.reshape(N_VOL, TILE_V)
    matches = owners[:, None, :] == jnp.arange(N_PIX, dtype=jnp.int32)[None, :, None]
    owner_ranking = jnp.cumsum(matches.astype(jnp.int32), axis=2, dtype=jnp.int32) - 1
    owner_rank = jnp.sum(jnp.where(matches, owner_ranking, 0), axis=1, dtype=jnp.int32)
    vol_ids = jnp.arange(N_VOL, dtype=jnp.int32)[:, None]
    destination = ((vol_ids * N_PIX + owners) * OWN_MAX + owner_rank).astype(jnp.int32)
    owned_tiles = jnp.zeros((DEVICES * OWN_MAX, CHANNELS * PIX_TILE), jnp.float32)
    owned_tiles = owned_tiles.at[destination.reshape(TILES)].set(shell_map)
    return owned_tiles, shell_map
```

```python
import functools

import jax
import jax.numpy as jnp
from jax import lax
from jax.experimental import pallas as pl
from jax.experimental.pallas import tpu as pltpu
from jax.sharding import PartitionSpec as P

MESH = pl.DeviceIdType.MESH
F32 = jnp.float32
BF16 = jnp.bfloat16

LANES = 128
ENTRIES = 16384
SLOTS = 1024
N_VOL = 16
SIDE = 4
BLOCK_TILES = 2048
CAP = 128
OWN_MAX = 512

STEP = 2048
SPAN = 256
WINDOW = 32
MSG = 2 * CAP + 8
FIRST = CAP + 8


def dot(a, b):
    return jnp.dot(a, b, preferred_element_type=F32)


def iota(shape, dim):
    return lax.broadcasted_iota(jnp.int32, shape, dim)


def halves(x):
    high = x.astype(BF16)
    return high, (x - high.astype(F32)).astype(BF16)


def project_kernel(slot_s, kernel_ref, pressure_ref, velocity_ref, slot_ref, tile_ref, send_ref, acc, rhs):
    step = pl.program_id(0)

    @pl.when(step == 0)
    def _():
        acc[...] = jnp.zeros_like(acc)

    thermal = pressure_ref[...].astype(F32)
    kinetic = velocity_ref[...].astype(F32)
    slots = slot_ref[...]
    rows = iota((WINDOW, LANES), 0)

    def products(i, base):
        top, low = [], []
        for h in range(SPAN // LANES):
            r = i * (SPAN // LANES) + h
            match = rows == slots[r : r + 1, :] - base
            top.append(jnp.where(match, thermal[r : r + 1, :], 0.0))
            low.append(jnp.where(match, kinetic[r : r + 1, :], 0.0))
        weights = jnp.concatenate([jnp.concatenate(top, 1), jnp.concatenate(low, 1)], 0)
        return dot(weights.astype(BF16), kernel_ref[i * SPAN : (i + 1) * SPAN, :])

    def add(base, value):
        acc[0, pl.ds(base, WINDOW), :] += value[:WINDOW]
        acc[1, pl.ds(base, WINDOW), :] += value[WINDOW:]

    bases, lasts, values = [], [], []
    for i in range(STEP // SPAN):
        r = i * (SPAN // LANES)
        bases.append(pl.multiple_of((slot_s[r, 0] // 8) * 8, 8))
        lasts.append(slot_s[r + SPAN // LANES - 1, LANES - 1])
        values.append(products(i, bases[i]))
    for i in range(STEP // SPAN):
        add(bases[i], values[i])
    for i in range(STEP // SPAN):

        @pl.loop(1, (lasts[i] - bases[i]) // WINDOW + 1)
        def _(w, i=i):
            base = pl.multiple_of(bases[i] + w * WINDOW, 8)
            add(base, products(i, base))

    @pl.when(step == pl.num_programs(0) - 1)
    def _():
        tiles = tile_ref[...]
        block = tiles // BLOCK_TILES
        within = tiles - block * BLOCK_TILES
        groups = SLOTS // LANES
        match = jnp.concatenate([(block == v).astype(F32) for v in range(N_VOL)], 0).astype(BF16)
        r, c = iota((LANES, LANES), 0), iota((LANES, LANES), 1)
        before = (r < c).astype(F32).astype(BF16)
        above = ((c < r) & (c // groups == r // groups)).astype(F32).astype(BF16)
        ones = jnp.ones((LANES, LANES), BF16)
        rank = dot(match, before) + dot(dot(above, match).astype(BF16), ones)
        key = jnp.where(match.astype(F32) > 0, rank, -1.0)
        for ch in range(2):
            high, low = halves(acc[ch, :SLOTS, :])
            rhs[:, ch * LANES : (ch + 1) * LANES] = high
            rhs[:, (ch + 2) * LANES : (ch + 3) * LANES] = low
        upper, lower = within // 64, within % 64
        place = r.astype(F32)
        which = iota((8, LANES), 0)
        codes = []
        for g in range(groups):
            codes.append(
                jnp.where(
                    which == 0,
                    upper[g : g + 1, :],
                    jnp.where(which == 1, lower[g : g + 1, :], jnp.where(which == 2, 1, 0)),
                )
            )
        code = jnp.concatenate(codes, 1).astype(F32).astype(BF16)
        for v in range(N_VOL):
            chosen = jnp.concatenate(
                [
                    (place == key[v * groups + g : v * groups + g + 1, :]).astype(F32).astype(BF16)
                    for g in range(groups)
                ],
                1,
            )
            out = dot(chosen, rhs[...])
            send_ref[v, :CAP, :] = out[:, :LANES] + out[:, 2 * LANES : 3 * LANES]
            send_ref[v, FIRST:, :] = out[:, LANES : 2 * LANES] + out[:, 3 * LANES :]
            ids = lax.dot_general(code, chosen, (((1,), (1,)), ((), ())), preferred_element_type=F32)
            tile = ids[0:1] * 64.0 + ids[1:2] + ids[2:3] - 1.0
            send_ref[v, CAP:FIRST, :] = jnp.broadcast_to(tile, (8, LANES))


def project(kernel, pressure, velocity, entry_slot, slot_tile):
    rows = STEP // LANES
    return pl.pallas_call(
        project_kernel,
        grid=(ENTRIES // STEP,),
        out_shape=jax.ShapeDtypeStruct((N_VOL, MSG, LANES), F32),
        in_specs=[
            pl.BlockSpec((rows, LANES), lambda g: (g, 0), memory_space=pltpu.SMEM),
            pl.BlockSpec((STEP, LANES), lambda g: (g, 0)),
            pl.BlockSpec((rows, LANES), lambda g: (g, 0)),
            pl.BlockSpec((rows, LANES), lambda g: (g, 0)),
            pl.BlockSpec((rows, LANES), lambda g: (g, 0)),
            pl.BlockSpec((SLOTS // LANES, LANES), lambda g: (0, 0)),
        ],
        out_specs=pl.BlockSpec((N_VOL, MSG, LANES), lambda g: (0, 0, 0)),
        scratch_shapes=[
            pltpu.VMEM((2, SLOTS + WINDOW + 8, LANES), F32),
            pltpu.VMEM((SLOTS, 4 * LANES), BF16),
        ],
        compiler_params=pltpu.CompilerParams(dimension_semantics=("arbitrary",)),
        name="project",
    )(entry_slot, kernel, pressure, velocity, entry_slot, slot_tile)


GROUP = 4
HALF = BLOCK_TILES // 2
PIECE = HALF // SIDE
TALL = 256


def exchange_kernel(
    send, out, recv, acc, other, parts, rhs,
    p1s, p1r, d2s, d2r, rss, rsr, ags, agr, fws, fwr,
):
    vol = lax.axis_index("vol")
    pix = lax.axis_index("pix")
    x, core = pix // 2, pix % 2
    y, z = vol // SIDE, vol % SIDE

    def vol_to(k):
        return {"vol": lax.rem(y + k // SIDE, SIDE) * SIDE + lax.rem(z + k % SIDE, SIDE)}

    def pix_to(k):
        return {"pix": lax.rem(x + k, SIDE) * 2 + core}

    partner = {"pix": x * 2 + 1 - core}
    peers = [vol_to(k) for k in range(1, N_VOL)] + [pix_to(k) for k in range(1, SIDE)] + [partner]
    barrier = pltpu.get_barrier_semaphore()
    for peer in peers:
        pl.semaphore_signal(barrier, inc=1, device_id=peer, device_id_type=MESH)
    pl.semaphore_wait(barrier, len(peers))

    started = []

    def copy(src, dst, s, r, peer):
        c = pltpu.make_async_remote_copy(
            src_ref=src, dst_ref=dst, send_sem=s, recv_sem=r, device_id=peer, device_id_type=MESH
        )
        c.start()
        started.append(c)
        return c

    spans = ((0, FIRST), (FIRST, CAP))
    rows_of = (0, FIRST)
    first = [[None] * N_VOL for _ in range(2)]
    for ch in range(2):
        begin, size = spans[ch]
        for k in range(1, N_VOL):
            peer = vol_to(k)
            first[ch][k] = copy(
                send.at[peer["vol"], pl.ds(begin, size)],
                recv.at[k, pl.ds(begin, size)],
                p1s.at[ch, k], p1r.at[ch, k], peer,
            )

    def combine(ch, group):
        ids = []
        for n in range(GROUP):
            k = group * GROUP + n
            if k:
                first[ch][k].wait_recv()
                ids.append(recv[k, CAP : CAP + 1, :])
                rows = recv[k, rows_of[ch] : rows_of[ch] + CAP, :]
            else:
                ids.append(send[vol, CAP : CAP + 1, :])
                rows = send[vol, rows_of[ch] : rows_of[ch] + CAP, :]
            high, low = halves(rows)
            rhs[n * CAP : (n + 1) * CAP, :LANES] = high
            rhs[n * CAP : (n + 1) * CAP, LANES:] = low

        @pl.loop(0, BLOCK_TILES // TALL)
        def _(t):
            at = pl.multiple_of(t * TALL, TALL)
            tile = (iota((TALL, LANES), 0) + at).astype(F32)
            chosen = jnp.concatenate([(tile == i).astype(F32).astype(BF16) for i in ids], 1)
            both = dot(chosen, rhs[...])
            total = both[:, :LANES] + both[:, LANES:]
            if group:
                total += acc[ch, pl.ds(at, TALL), :]
            acc[ch, pl.ds(at, TALL), :] = total

    mine = core * HALF
    theirs = HALF - mine

    def swap(ch):
        return copy(acc.at[ch, pl.ds(theirs, HALF)], other.at[ch], d2s.at[ch], d2r.at[ch], partner)

    def reduce_start(ch, swapped):
        swapped.wait_recv()
        acc[ch, pl.ds(mine, HALF), :] += other[ch]
        copies = []
        for k in range(1, SIDE):
            at = pl.multiple_of(mine + lax.rem(x + k, SIDE) * PIECE, PIECE)
            copies.append(
                copy(acc.at[ch, pl.ds(at, PIECE)], parts.at[ch, k - 1], rss.at[ch, k - 1], rsr.at[ch, k - 1], pix_to(k))
            )
        return copies

    here = pl.multiple_of(mine + x * PIECE, PIECE)

    def gather_start(ch, copies):
        total = acc[ch, pl.ds(here, PIECE), :]
        for k in range(1, SIDE):
            copies[k - 1].wait_recv()
            total += parts[ch, k - 1]
        out[ch, pl.ds(here, PIECE), :] = total
        block = out.at[ch, pl.ds(here, PIECE)]
        gathers = [
            copy(block, block, ags.at[ch, k - 1], agr.at[ch, k - 1], pix_to(k)) for k in range(1, SIDE)
        ]
        return gathers, [copy(block, block, fws.at[ch, 0], fwr.at[ch, 0], partner)]

    def forward(ch, gathers, sent):
        for k in range(1, SIDE):
            gathers[k - 1].wait_recv()
            at = pl.multiple_of(mine + lax.rem(x - k + SIDE, SIDE) * PIECE, PIECE)
            block = out.at[ch, pl.ds(at, PIECE)]
            sent.append(copy(block, block, fws.at[ch, k], fwr.at[ch, k], partner))
        return sent

    groups = N_VOL // GROUP
    for g in range(groups):
        combine(0, g)
    s0 = swap(0)
    combine(1, 0)
    r0 = reduce_start(0, s0)
    combine(1, 1)
    a0, f0 = gather_start(0, r0)
    combine(1, 2)
    f0 = forward(0, a0, f0)
    combine(1, 3)
    s1 = swap(1)
    r1 = reduce_start(1, s1)
    a1, f1 = gather_start(1, r1)
    f1 = forward(1, a1, f1)
    for c in f0 + f1:
        c.wait_recv()
    for c in started:
        c.wait_send()


def exchange(send):
    vmem = pl.BlockSpec(memory_space=pltpu.VMEM)
    dma = pltpu.SemaphoreType.DMA
    return pl.pallas_call(
        exchange_kernel,
        out_shape=jax.ShapeDtypeStruct((2, BLOCK_TILES, LANES), F32),
        in_specs=[vmem],
        out_specs=vmem,
        scratch_shapes=[
            pltpu.VMEM((N_VOL, MSG, LANES), F32),
            pltpu.VMEM((2, BLOCK_TILES, LANES), F32),
            pltpu.VMEM((2, HALF, LANES), F32),
            pltpu.VMEM((2, SIDE - 1, PIECE, LANES), F32),
            pltpu.VMEM((GROUP * CAP, 2 * LANES), BF16),
            dma((2, N_VOL)), dma((2, N_VOL)),
            dma((2,)), dma((2,)),
            dma((2, SIDE - 1)), dma((2, SIDE - 1)),
            dma((2, SIDE - 1)), dma((2, SIDE - 1)),
            dma((2, SIDE)), dma((2, SIDE)),
        ],
        compiler_params=pltpu.CompilerParams(collective_id=0, has_side_effects=True),
        name="exchange",
    )(send)


def finish_kernel(map_ref, owner_ref, owned_ref, shell_ref, rhs):
    vol = lax.axis_index("vol")
    pix = lax.axis_index("pix")
    rows = BLOCK_TILES // LANES
    owner = owner_ref[pl.ds(pl.multiple_of(vol * rows, rows), rows), :]
    match = (owner == pix).astype(F32).astype(BF16)
    before = (iota((LANES, LANES), 0) < iota((LANES, LANES), 1)).astype(F32).astype(BF16)
    above = (iota((rows, rows), 1) < iota((rows, rows), 0)).astype(F32).astype(BF16)
    ones = jnp.ones((LANES, LANES), BF16)
    rank = dot(match, before) + dot(dot(above, match).astype(BF16), ones)
    key = jnp.where(match.astype(F32) > 0, rank, -1.0)
    for ch in range(2):
        value = map_ref[ch]
        shell_ref[:, ch * LANES : (ch + 1) * LANES] = value
        high, low = halves(value)
        rhs[:, ch * LANES : (ch + 1) * LANES] = high
        rhs[:, (ch + 2) * LANES : (ch + 3) * LANES] = low
    for t in range(OWN_MAX // TALL):
        place = (iota((TALL, LANES), 0) + t * TALL).astype(F32)
        chosen = jnp.concatenate(
            [(place == key[g : g + 1, :]).astype(F32).astype(BF16) for g in range(rows)], 1
        )
        both = dot(chosen, rhs[...])
        owned_ref[t * TALL : (t + 1) * TALL, :] = both[:, : 2 * LANES] + both[:, 2 * LANES :]


def finish(block_map, tile_owner):
    vmem = pl.BlockSpec(memory_space=pltpu.VMEM)
    return pl.pallas_call(
        finish_kernel,
        out_shape=(
            jax.ShapeDtypeStruct((OWN_MAX, 2 * LANES), F32),
            jax.ShapeDtypeStruct((BLOCK_TILES, 2 * LANES), F32),
        ),
        in_specs=[vmem, vmem],
        out_specs=(vmem, vmem),
        scratch_shapes=[pltpu.VMEM((BLOCK_TILES, 4 * LANES), BF16)],
        name="finish",
    )(block_map, tile_owner)


def shards(kernel, pressure, velocity, entry_slot, slot_tile, tile_owner):
    square = (ENTRIES // LANES, LANES)
    send = project(
        kernel,
        pressure.reshape(square),
        velocity.reshape(square),
        entry_slot.reshape(square),
        slot_tile.reshape(SLOTS // LANES, LANES),
    )
    block_map = exchange(send)
    return finish(block_map, tile_owner.reshape(-1, LANES))


def solution(mesh):
    in_specs = (
        P(("vol", "pix"), None),
        P(("vol", "pix")),
        P(("vol", "pix")),
        P(("vol", "pix"), None),
        P(("vol", "pix"), None),
        P(),
    )
    out_specs = (P(("vol", "pix"), None), P("vol", None))
    return jax.shard_map(shards, mesh=mesh, in_specs=in_specs, out_specs=out_specs, check_vma=False)
```

```python
import functools

import jax
import jax.numpy as jnp
from jax import lax
from jax.experimental import pallas as pl
from jax.experimental.pallas import tpu as pltpu
from jax.sharding import PartitionSpec as P

MESH = pl.DeviceIdType.MESH
F32 = jnp.float32
BF16 = jnp.bfloat16

LANES = 128
ENTRIES = 16384
SLOTS = 1024
N_VOL = 16
SIDE = 4
BLOCK_TILES = 2048
CAP = 128
OWN_MAX = 512

STEP = 2048
SPAN = 256
WINDOW = 32
MSG = 2 * CAP + 8
FIRST = CAP + 8


def dot(a, b):
    return jnp.dot(a, b, preferred_element_type=F32)


def iota(shape, dim):
    return lax.broadcasted_iota(jnp.int32, shape, dim)


def halves(x):
    high = x.astype(BF16)
    return high, (x - high.astype(F32)).astype(BF16)


def project_kernel(slot_s, kernel_ref, pressure_ref, velocity_ref, slot_ref, tile_ref, rhs_ref, key_ref, code_ref, acc):
    step = pl.program_id(0)

    @pl.when(step == 0)
    def _():
        acc[...] = jnp.zeros_like(acc)

    thermal = pressure_ref[...].astype(F32)
    kinetic = velocity_ref[...].astype(F32)
    slots = slot_ref[...]
    rows = iota((WINDOW, LANES), 0)

    def products(i, base):
        top, low = [], []
        for h in range(SPAN // LANES):
            r = i * (SPAN // LANES) + h
            match = rows == slots[r : r + 1, :] - base
            top.append(jnp.where(match, thermal[r : r + 1, :], 0.0))
            low.append(jnp.where(match, kinetic[r : r + 1, :], 0.0))
        weights = jnp.concatenate([jnp.concatenate(top, 1), jnp.concatenate(low, 1)], 0)
        return dot(weights.astype(BF16), kernel_ref[i * SPAN : (i + 1) * SPAN, :])

    def add(base, value):
        acc[0, pl.ds(base, WINDOW), :] += value[:WINDOW]
        acc[1, pl.ds(base, WINDOW), :] += value[WINDOW:]

    bases, lasts, values = [], [], []
    for i in range(STEP // SPAN):
        r = i * (SPAN // LANES)
        bases.append(pl.multiple_of((slot_s[r, 0] // 8) * 8, 8))
        lasts.append(slot_s[r + SPAN // LANES - 1, LANES - 1])
        values.append(products(i, bases[i]))
    for i in range(STEP // SPAN):
        add(bases[i], values[i])
    for i in range(STEP // SPAN):

        @pl.loop(1, (lasts[i] - bases[i]) // WINDOW + 1)
        def _(w, i=i):
            base = pl.multiple_of(bases[i] + w * WINDOW, 8)
            add(base, products(i, base))

    @pl.when(step == pl.num_programs(0) - 1)
    def _():
        tiles = tile_ref[...]
        block = tiles // BLOCK_TILES
        within = tiles - block * BLOCK_TILES
        groups = SLOTS // LANES
        match = jnp.concatenate([(block == v).astype(F32) for v in range(N_VOL)], 0).astype(BF16)
        r, c = iota((LANES, LANES), 0), iota((LANES, LANES), 1)
        before = (r < c).astype(F32).astype(BF16)
        above = ((c < r) & (c // groups == r // groups)).astype(F32).astype(BF16)
        ones = jnp.ones((LANES, LANES), BF16)
        rank = dot(match, before) + dot(dot(above, match).astype(BF16), ones)
        key_ref[...] = jnp.where(match.astype(F32) > 0, rank, -1.0)
        for ch in range(2):
            high, low = halves(acc[ch, :SLOTS, :])
            rhs_ref[:, ch * LANES : (ch + 1) * LANES] = high
            rhs_ref[:, (ch + 2) * LANES : (ch + 3) * LANES] = low
        upper, lower = within // 64, within % 64
        which = iota((8, LANES), 0)
        for g in range(groups):
            here = slice(g, g + 1)
            rest = jnp.where(which == 2, 1, 0)
            code = jnp.where(which == 0, upper[here], jnp.where(which == 1, lower[here], rest))
            code_ref[:, g * LANES : (g + 1) * LANES] = code.astype(F32).astype(BF16)


def project(kernel, pressure, velocity, entry_slot, slot_tile):
    rows = STEP // LANES
    outs = (((SLOTS, 4 * LANES), BF16), ((LANES, LANES), F32), ((8, SLOTS), BF16))
    return pl.pallas_call(
        project_kernel,
        grid=(ENTRIES // STEP,),
        out_shape=tuple(jax.ShapeDtypeStruct(*o) for o in outs),
        in_specs=[
            pl.BlockSpec((rows, LANES), lambda g: (g, 0), memory_space=pltpu.SMEM),
            pl.BlockSpec((STEP, LANES), lambda g: (g, 0)),
            pl.BlockSpec((rows, LANES), lambda g: (g, 0)),
            pl.BlockSpec((rows, LANES), lambda g: (g, 0)),
            pl.BlockSpec((rows, LANES), lambda g: (g, 0)),
            pl.BlockSpec((SLOTS // LANES, LANES), lambda g: (0, 0)),
        ],
        out_specs=tuple(pl.BlockSpec(o[0], lambda g: (0, 0)) for o in outs),
        scratch_shapes=[pltpu.VMEM((2, SLOTS + WINDOW + 8, LANES), F32)],
        compiler_params=pltpu.CompilerParams(dimension_semantics=("arbitrary",)),
        name="project",
    )(entry_slot, kernel, pressure, velocity, entry_slot, slot_tile)


GROUP = 4
SUBS = 2
HALF = BLOCK_TILES // 2
SUB = HALF // SUBS
PIECE = SUB // SIDE
TALL = 256
ORDER = tuple(range(N_VOL))


def equal(place, row):
    return jnp.where(place == row, jnp.ones((), BF16), jnp.zeros((), BF16))


def exchange_kernel(
    partial, keys, code, out, send, recv, acc, other, parts, rhs, hot,
    p1s, p1r, d2s, d2r, rss, rsr, ags, agr, fws, fwr,
):
    vol = lax.axis_index("vol")
    pix = lax.axis_index("pix")
    x, core = pix // 2, pix % 2
    y, z = vol // SIDE, vol % SIDE

    def vol_to(k):
        return lax.rem(y + k // SIDE, SIDE) * SIDE + lax.rem(z + k % SIDE, SIDE)

    def pix_to(k):
        return {"pix": lax.rem(x + k, SIDE) * 2 + core}

    partner = {"pix": x * 2 + 1 - core}
    peers = [{"vol": vol_to(k)} for k in range(1, N_VOL)] + [pix_to(k) for k in range(1, SIDE)] + [partner]
    barrier = pltpu.get_barrier_semaphore()
    for peer in peers:
        pl.semaphore_signal(barrier, inc=1, device_id=peer, device_id_type=MESH)

    started = []

    def copy(src, dst, s, r, peer):
        c = pltpu.make_async_remote_copy(
            src_ref=src, dst_ref=dst, send_sem=s, recv_sem=r, device_id=peer, device_id_type=MESH
        )
        c.start()
        started.append(c)
        return c

    spans = ((0, FIRST), (FIRST, CAP))
    rows_of = (0, FIRST)
    first = [[None] * N_VOL for _ in range(2)]

    def launch(ch, k):
        begin, size = spans[ch]
        to = vol_to(k)
        first[ch][k] = copy(
            send.at[k, pl.ds(begin, size)],
            recv.at[k, pl.ds(begin, size)],
            p1s.at[ch, k], p1r.at[ch, k], {"vol": to},
        )

    place = iota((CAP, LANES), 0).astype(F32).astype(BF16)

    def message(k):
        groups = SLOTS // LANES
        key = keys[pl.ds(pl.multiple_of(vol_to(k) * groups, groups), groups), :]
        chosen = jnp.concatenate(
            [equal(place, key[g : g + 1, :].astype(BF16)) for g in range(groups)], 1
        )
        both = dot(chosen, partial[...])
        send[k, :CAP, :] = both[:, :LANES] + both[:, 2 * LANES : 3 * LANES]
        send[k, FIRST:, :] = both[:, LANES : 2 * LANES] + both[:, 3 * LANES :]
        ids = lax.dot_general(code[...], chosen, (((1,), (1,)), ((), ())), preferred_element_type=F32)
        tile = ids[0:1] * 64.0 + ids[1:2] + ids[2:3] - 1.0
        send[k, CAP:FIRST, :] = jnp.broadcast_to(tile, (8, LANES))

    todo = ORDER[1:] + ORDER[:1]
    with jax.named_scope("messages"):
        for n, k in enumerate(todo):
            message(k)
            if n == 0:
                pl.semaphore_wait(barrier, len(peers))
            else:
                launch(0, todo[n - 1])
        for k in ORDER[1:]:
            launch(1, k)

    tall = iota((TALL, LANES), 0).astype(F32).astype(BF16)
    mine = core * HALF
    theirs = HALF - mine
    turn = GROUP * CAP

    def load(ch, group):
        ids = []
        for n in range(GROUP):
            k = ORDER[group * GROUP + n]
            source = recv if k else send
            if k:
                first[ch][k].wait_recv()
            ids.append(source[k, CAP : CAP + 1, :])
            high, low = halves(source[k, rows_of[ch] : rows_of[ch] + CAP, :])
            rhs[n * CAP : (n + 1) * CAP, :LANES] = high
            rhs[n * CAP : (n + 1) * CAP, LANES:] = low
        return ids

    def tiles(ch, group, ids, begin, size):
        columns = slice(group * turn, (group + 1) * turn)

        @pl.loop(0, size // TALL)
        def _(t):
            at = pl.multiple_of(begin + t * TALL, TALL)
            if ch == 0:
                pieces = []
                for i in ids:
                    local = i - at.astype(F32)
                    local = jnp.where((local >= 0) & (local < TALL), local, -1.0)
                    pieces.append(equal(tall, local.astype(BF16)))
                chosen = jnp.concatenate(pieces, 1)
                hot[pl.ds(at, TALL), columns] = chosen
            else:
                chosen = hot[pl.ds(at, TALL), columns]
            both = dot(chosen, rhs[...])
            total = both[:, :LANES] + both[:, LANES:]
            if group:
                total += acc[ch, pl.ds(at, TALL), :]
            acc[ch, pl.ds(at, TALL), :] = total

    def combine(ch, group):
        with jax.named_scope(f"load{ch}{group}"):
            ids = load(ch, group)
        with jax.named_scope(f"combine{ch}{group}"):
            tiles(ch, group, ids, 0, BLOCK_TILES)

    def combine_swap(ch, group):
        with jax.named_scope(f"load{ch}{group}"):
            ids = load(ch, group)
        copies = []
        with jax.named_scope(f"combine{ch}{group}"):
            for s in range(SUBS):
                tiles(ch, group, ids, theirs + s * SUB, SUB)
                at = pl.multiple_of(theirs + s * SUB, SUB)
                copies.append(
                    copy(acc.at[ch, pl.ds(at, SUB)], other.at[ch, s], d2s.at[ch, s], d2r.at[ch, s], partner)
                )
            tiles(ch, group, ids, mine, HALF)
        return copies

    def reduce_start(ch, s, swapped):
        with jax.named_scope(f"reduce{ch}{s}"):
            swapped.wait_recv()
            acc[ch, pl.ds(pl.multiple_of(mine + s * SUB, SUB), SUB), :] += other[ch, s]
            copies = []
            for k in (2, 1, 3):
                at = pl.multiple_of(mine + s * SUB + lax.rem(x + k, SIDE) * PIECE, PIECE)
                copies.append(
                    copy(
                        acc.at[ch, pl.ds(at, PIECE)], parts.at[ch, s, k - 1],
                        rss.at[ch, s, k - 1], rsr.at[ch, s, k - 1], pix_to(k),
                    )
                )
        return copies

    def gather_start(ch, s, copies):
        with jax.named_scope(f"gather{ch}{s}"):
            here = pl.multiple_of(mine + s * SUB + x * PIECE, PIECE)
            for c in copies:
                c.wait_recv()
            total = acc[ch, pl.ds(here, PIECE), :]
            for k in range(1, SIDE):
                total += parts[ch, s, k - 1]
            out[ch, pl.ds(here, PIECE), :] = total
            block = out.at[ch, pl.ds(here, PIECE)]
            gathers = [
                (k, copy(block, block, ags.at[ch, s, k - 1], agr.at[ch, s, k - 1], pix_to(k))) for k in (2, 1, 3)
            ]
        return gathers, [copy(block, block, fws.at[ch, s, 0], fwr.at[ch, s, 0], partner)]

    def forward(ch, s, started_gathers):
        gathers, sent = started_gathers
        with jax.named_scope(f"forward{ch}{s}"):
            for k, c in (gathers[1], gathers[2], gathers[0]):
                c.wait_recv()
                at = pl.multiple_of(mine + s * SUB + lax.rem(x - k + SIDE, SIDE) * PIECE, PIECE)
                block = out.at[ch, pl.ds(at, PIECE)]
                sent.append(copy(block, block, fws.at[ch, s, k], fwr.at[ch, s, k], partner))
        return sent

    for g in range(3):
        combine(0, g)
    s0 = combine_swap(0, 3)
    combine(1, 0)
    r0 = [reduce_start(0, s, s0[s]) for s in range(SUBS)]
    combine(1, 1)
    combine(1, 2)
    g0 = [gather_start(0, s, r0[s]) for s in range(SUBS)]
    s1 = combine_swap(1, 3)
    r1 = [reduce_start(1, s, s1[s]) for s in range(SUBS)]
    f0 = [forward(0, s, g0[s]) for s in range(SUBS)]
    g1 = [gather_start(1, s, r1[s]) for s in range(SUBS)]
    f1 = [forward(1, s, g1[s]) for s in range(SUBS)]
    with jax.named_scope("last"):
        for f in f0 + f1:
            for c in f:
                c.wait_recv()
        for c in started:
            c.wait_send()


def exchange(partial, keys, code):
    vmem = pl.BlockSpec(memory_space=pltpu.VMEM)
    dma = pltpu.SemaphoreType.DMA
    return pl.pallas_call(
        exchange_kernel,
        out_shape=jax.ShapeDtypeStruct((2, BLOCK_TILES, LANES), F32),
        in_specs=[vmem] * 3,
        out_specs=vmem,
        scratch_shapes=[
            pltpu.VMEM((N_VOL, MSG, LANES), F32),
            pltpu.VMEM((N_VOL, MSG, LANES), F32),
            pltpu.VMEM((2, BLOCK_TILES, LANES), F32),
            pltpu.VMEM((2, SUBS, SUB, LANES), F32),
            pltpu.VMEM((2, SUBS, SIDE - 1, PIECE, LANES), F32),
            pltpu.VMEM((GROUP * CAP, 2 * LANES), BF16),
            pltpu.VMEM((BLOCK_TILES, N_VOL * CAP), BF16),
            dma((2, N_VOL)), dma((2, N_VOL)),
            dma((2, SUBS)), dma((2, SUBS)),
            dma((2, SUBS, SIDE - 1)), dma((2, SUBS, SIDE - 1)),
            dma((2, SUBS, SIDE - 1)), dma((2, SUBS, SIDE - 1)),
            dma((2, SUBS, SIDE)), dma((2, SUBS, SIDE)),
        ],
        compiler_params=pltpu.CompilerParams(collective_id=0, has_side_effects=True),
        name="exchange",
    )(partial, keys, code)


def finish_kernel(map_ref, owner_ref, owned_ref, shell_ref, rhs):
    vol = lax.axis_index("vol")
    pix = lax.axis_index("pix")
    rows = BLOCK_TILES // LANES
    owner = owner_ref[pl.ds(pl.multiple_of(vol * rows, rows), rows), :]
    match = (owner == pix).astype(F32).astype(BF16)
    before = (iota((LANES, LANES), 0) < iota((LANES, LANES), 1)).astype(F32).astype(BF16)
    above = (iota((rows, rows), 1) < iota((rows, rows), 0)).astype(F32).astype(BF16)
    ones = jnp.ones((LANES, LANES), BF16)
    rank = dot(match, before) + dot(dot(above, match).astype(BF16), ones)
    key = jnp.where(match.astype(F32) > 0, rank, -1.0)
    for ch in range(2):
        value = map_ref[ch]
        shell_ref[:, ch * LANES : (ch + 1) * LANES] = value
        high, low = halves(value)
        rhs[:, ch * LANES : (ch + 1) * LANES] = high
        rhs[:, (ch + 2) * LANES : (ch + 3) * LANES] = low
    for t in range(OWN_MAX // TALL):
        place = (iota((TALL, LANES), 0) + t * TALL).astype(F32)
        chosen = jnp.concatenate(
            [(place == key[g : g + 1, :]).astype(F32).astype(BF16) for g in range(rows)], 1
        )
        both = dot(chosen, rhs[...])
        owned_ref[t * TALL : (t + 1) * TALL, :] = both[:, : 2 * LANES] + both[:, 2 * LANES :]


def finish(block_map, tile_owner):
    vmem = pl.BlockSpec(memory_space=pltpu.VMEM)
    return pl.pallas_call(
        finish_kernel,
        out_shape=(
            jax.ShapeDtypeStruct((OWN_MAX, 2 * LANES), F32),
            jax.ShapeDtypeStruct((BLOCK_TILES, 2 * LANES), F32),
        ),
        in_specs=[vmem, vmem],
        out_specs=(vmem, vmem),
        scratch_shapes=[pltpu.VMEM((BLOCK_TILES, 4 * LANES), BF16)],
        name="finish",
    )(block_map, tile_owner)


def shards(kernel, pressure, velocity, entry_slot, slot_tile, tile_owner):
    square = (ENTRIES // LANES, LANES)
    partial, keys, code = project(
        kernel,
        pressure.reshape(square),
        velocity.reshape(square),
        entry_slot.reshape(square),
        slot_tile.reshape(SLOTS // LANES, LANES),
    )
    block_map = exchange(partial, keys, code)
    return finish(block_map, tile_owner.reshape(-1, LANES))


def solution(mesh):
    in_specs = (
        P(("vol", "pix"), None),
        P(("vol", "pix")),
        P(("vol", "pix")),
        P(("vol", "pix"), None),
        P(("vol", "pix"), None),
        P(),
    )
    out_specs = (P(("vol", "pix"), None), P("vol", None))
    return jax.shard_map(shards, mesh=mesh, in_specs=in_specs, out_specs=out_specs, check_vma=False)
```

```python
import functools

import jax
import jax.numpy as jnp
from jax import lax
from jax.experimental import pallas as pl
from jax.experimental.pallas import tpu as pltpu
from jax.sharding import PartitionSpec as P

MESH = pl.DeviceIdType.MESH
F32 = jnp.float32
BF16 = jnp.bfloat16

LANES = 128
ENTRIES = 16384
SLOTS = 1024
N_VOL = 16
SIDE = 4
BLOCK_TILES = 2048
CAP = 128
OWN_MAX = 512

STEP = 2048
SPAN = 256
WINDOW = 32
MSG = 2 * CAP + 8
FIRST = CAP + 8


def dot(a, b):
    return jnp.dot(a, b, preferred_element_type=F32)


def iota(shape, dim):
    return lax.broadcasted_iota(jnp.int32, shape, dim)


def halves(x):
    high = x.astype(BF16)
    return high, (x - high.astype(F32)).astype(BF16)


def equal(place, row):
    return jnp.where(place == row, jnp.ones((), BF16), jnp.zeros((), BF16))


def project_kernel(
    kernel_h, pressure_h, velocity_h, slot_h, tile_h, rhs_ref, key_ref, ids_ref,
    weights, pressure, velocity, slot_v, tile_v, slot_s, acc, sems, chunk_sems,
):
    steps = ENTRIES // STEP
    rows = STEP // LANES
    small = [
        pltpu.make_async_copy(a, b, sems.at[n])
        for n, (a, b) in enumerate(
            (
                (tile_h, tile_v), (slot_h, slot_s), (slot_h, slot_v),
                (pressure_h, pressure), (velocity_h, velocity),
            )
        )
    ]
    for c in small:
        c.start()

    def chunk(g):
        span = pl.ds(pl.multiple_of(g * STEP, STEP), STEP)
        return pltpu.make_async_copy(kernel_h.at[span], weights.at[span], chunk_sems.at[g])

    for g in range(steps):
        chunk(g).start()
    acc[...] = jnp.zeros_like(acc)

    small[0].wait()
    tiles = tile_v[...]
    block = tiles // BLOCK_TILES
    within = tiles - block * BLOCK_TILES
    groups = SLOTS // LANES
    match = jnp.concatenate([(block == v).astype(F32) for v in range(N_VOL)], 0)
    r, c = iota((LANES, LANES), 0), iota((LANES, LANES), 1)
    before = (r < c).astype(F32).astype(BF16)
    above = ((c < r) & (c // groups == r // groups)).astype(F32).astype(BF16)
    ones = jnp.ones((LANES, LANES), BF16)
    packed = match.astype(BF16)
    rank = dot(packed, before) + dot(dot(above, packed).astype(BF16), ones)
    key_ref[...] = jnp.where(match > 0, rank, -1.0)
    own = jnp.zeros((groups, LANES), F32)
    for v in range(N_VOL):
        own += match[v * groups : (v + 1) * groups] * rank[v * groups : (v + 1) * groups]
    place = iota((LANES, LANES), 0).astype(F32).astype(BF16)
    spread = jnp.concatenate([equal(place, own[g : g + 1].astype(BF16)) for g in range(groups)], 1)
    vols = iota((N_VOL, LANES), 0)
    upper, lower = (within // 64).astype(F32), (within % 64).astype(F32)
    table = []
    for values in (upper, lower, jnp.ones_like(upper)):
        table.append(
            jnp.concatenate(
                [jnp.where(vols == block[g : g + 1], values[g : g + 1], 0.0) for g in range(groups)], 1
            )
        )
    table = jnp.concatenate(table, 0).astype(BF16)
    found = lax.dot_general(table, spread, (((1,), (1,)), ((), ())), preferred_element_type=F32)
    ids_ref[...] = found[:N_VOL] * 64.0 + found[N_VOL : 2 * N_VOL] + found[2 * N_VOL :] - 1.0

    for n in (1, 2, 3, 4):
        small[n].wait()
    lines = iota((WINDOW, LANES), 0)
    per = SPAN // LANES

    @pl.loop(0, steps)
    def _(g):
        chunk(g).wait()
        top = pl.multiple_of(g * rows, rows)
        thermal = pressure[pl.ds(top, rows), :].astype(F32)
        kinetic = velocity[pl.ds(top, rows), :].astype(F32)
        slots = slot_v[pl.ds(top, rows), :]

        def products(i, base):
            up, low = [], []
            for h in range(per):
                n = i * per + h
                match = lines == slots[n : n + 1, :] - base
                up.append(jnp.where(match, thermal[n : n + 1, :], 0.0))
                low.append(jnp.where(match, kinetic[n : n + 1, :], 0.0))
            amplitudes = jnp.concatenate([jnp.concatenate(up, 1), jnp.concatenate(low, 1)], 0)
            span = pl.ds(pl.multiple_of(g * STEP + i * SPAN, SPAN), SPAN)
            return dot(amplitudes.astype(BF16), weights[span, :])

        def add(base, value):
            acc[0, pl.ds(base, WINDOW), :] += value[:WINDOW]
            acc[1, pl.ds(base, WINDOW), :] += value[WINDOW:]

        count = STEP // SPAN
        bases, lasts = [], []
        for i in range(count):
            bases.append(pl.multiple_of((slot_s[top + i * per, 0] // 8) * 8, 8))
            lasts.append(slot_s[top + i * per + per - 1, LANES - 1])
        values = [products(i, bases[i]) for i in range(count)]
        for i in range(count):
            add(bases[i], values[i])
        for i in range(count):

            @pl.loop(1, (lasts[i] - bases[i]) // WINDOW + 1)
            def _(w, i=i):
                base = pl.multiple_of(bases[i] + w * WINDOW, 8)
                add(base, products(i, base))

    for ch in range(2):
        high, low = halves(acc[ch, :SLOTS, :])
        rhs_ref[:, 2 * ch * LANES : (2 * ch + 1) * LANES] = high
        rhs_ref[:, (2 * ch + 1) * LANES : (2 * ch + 2) * LANES] = low


def project(kernel, pressure, velocity, entry_slot, slot_tile):
    outs = (((SLOTS, 4 * LANES), BF16), ((LANES, LANES), F32), ((N_VOL, LANES), F32))
    square = (ENTRIES // LANES, LANES)
    return pl.pallas_call(
        project_kernel,
        out_shape=tuple(jax.ShapeDtypeStruct(*o) for o in outs),
        in_specs=[pl.BlockSpec(memory_space=pltpu.HBM)] * 5,
        out_specs=tuple(pl.BlockSpec(memory_space=pltpu.VMEM) for o in outs),
        scratch_shapes=[
            pltpu.VMEM((ENTRIES, LANES), BF16),
            pltpu.VMEM(square, BF16),
            pltpu.VMEM(square, BF16),
            pltpu.VMEM(square, jnp.int32),
            pltpu.VMEM((SLOTS // LANES, LANES), jnp.int32),
            pltpu.SMEM(square, jnp.int32),
            pltpu.VMEM((2, SLOTS + WINDOW + 8, LANES), F32),
            pltpu.SemaphoreType.DMA((5,)),
            pltpu.SemaphoreType.DMA((ENTRIES // STEP,)),
        ],
        compiler_params=pltpu.CompilerParams(vmem_limit_bytes=16 << 20),
        name="project",
    )(*(pltpu.with_memory_space_constraint(a, pltpu.HBM) for a in (kernel, pressure, velocity, entry_slot, slot_tile)))


GROUP = 4
SUBS = 2
HALF = BLOCK_TILES // 2
SUB = HALF // SUBS
PIECE = SUB // SIDE
TALL = 1024
BAND = 256
ORDER = (0, 1, 4, 3, 12, 5, 15, 7, 13, 2, 8, 6, 9, 10, 14, 11)
ROUND = 4


def exchange_kernel(
    partial, keys, ids_ref, out, send, recv, acc, other, parts, rhs, hot, pick,
    p1s, p1r, d2s, d2r, rss, rsr, ags, agr, fws, fwr,
):
    vol = lax.axis_index("vol")
    pix = lax.axis_index("pix")
    x, core = pix // 2, pix % 2
    y, z = vol // SIDE, vol % SIDE

    def vol_to(k):
        return lax.rem(y + k // SIDE, SIDE) * SIDE + lax.rem(z + k % SIDE, SIDE)

    def pix_to(k):
        return {"pix": lax.rem(x + k, SIDE) * 2 + core}

    partner = {"pix": x * 2 + 1 - core}
    peers = [{"vol": vol_to(k)} for k in range(1, N_VOL)] + [pix_to(k) for k in range(1, SIDE)] + [partner]
    barrier = pltpu.get_barrier_semaphore()
    for peer in peers:
        pl.semaphore_signal(barrier, inc=1, device_id=peer, device_id_type=MESH)

    started = []

    def copy(src, dst, s, r, peer):
        c = pltpu.make_async_remote_copy(
            src_ref=src, dst_ref=dst, send_sem=s, recv_sem=r, device_id=peer, device_id_type=MESH
        )
        c.start()
        started.append(c)
        return c

    spans = ((0, FIRST), (FIRST, CAP))
    rows_of = (0, FIRST)
    first = [[None] * N_VOL for _ in range(2)]

    def launch(ch, k):
        begin, size = spans[ch]
        to = vol_to(k)
        first[ch][k] = copy(
            send.at[k, pl.ds(begin, size)],
            recv.at[k, pl.ds(begin, size)],
            p1s.at[ch, k], p1r.at[ch, k], {"vol": to},
        )

    place = iota((CAP, LANES), 0).astype(F32).astype(BF16)
    groups = SLOTS // LANES

    def batch(ch, n, ks):
        here = slice(n * CAP, (n + len(ks)) * CAP)
        if ch == 0:
            for m, k in enumerate(ks):
                key = keys[pl.ds(pl.multiple_of(vol_to(k) * groups, groups), groups), :]
                pick[(n + m) * CAP : (n + m + 1) * CAP, :] = jnp.concatenate(
                    [equal(place, key[g : g + 1, :].astype(BF16)) for g in range(groups)], 1
                )
                send[k, CAP:FIRST, :] = jnp.broadcast_to(ids_ref[pl.ds(vol_to(k), 1), :], (8, LANES))
        both = dot(pick[here, :], partial[:, 2 * ch * LANES : 2 * (ch + 1) * LANES])
        total = both[:, :LANES] + both[:, LANES:]
        for m, k in enumerate(ks):
            send[k, rows_of[ch] : rows_of[ch] + CAP, :] = total[m * CAP : (m + 1) * CAP]

    todo = ORDER[1:] + ORDER[:1]
    waiting = []
    with jax.named_scope("messages"):
        for ch in range(2):
            for n in range(0, N_VOL, ROUND):
                ks = todo[n : n + ROUND]
                batch(ch, n, ks)
                if ch == 0 and n == 0:
                    pl.semaphore_wait(barrier, len(peers))
                for c, k in waiting:
                    launch(c, k)
                waiting = [(ch, k) for k in ks if k]
        for c, k in waiting:
            launch(c, k)

    band = iota((BAND, LANES), 0).astype(F32).astype(BF16)
    mine = core * HALF
    theirs = HALF - mine
    turn = GROUP * CAP

    def load(ch, group):
        ids = []
        for n in range(GROUP):
            k = ORDER[group * GROUP + n]
            source = recv if k else send
            if k:
                first[ch][k].wait_recv()
            ids.append(source[k, CAP : CAP + 1, :])
            high, low = halves(source[k, rows_of[ch] : rows_of[ch] + CAP, :])
            rhs[n * CAP : (n + 1) * CAP, :LANES] = high
            rhs[n * CAP : (n + 1) * CAP, LANES:] = low
        return ids

    def tiles(ch, group, ids, begin, count):
        columns = slice(group * turn, (group + 1) * turn)

        def one(t):
            at = pl.multiple_of(begin + t * TALL, TALL)
            if ch == 0:
                for b in range(TALL // BAND):
                    low = pl.multiple_of(at + b * BAND, BAND)
                    pieces = []
                    for i in ids:
                        local = i - low.astype(F32)
                        local = jnp.where((local >= 0) & (local < BAND), local, -1.0)
                        pieces.append(equal(band, local.astype(BF16)))
                    hot[pl.ds(low, BAND), columns] = jnp.concatenate(pieces, 1)
            both = dot(hot[pl.ds(at, TALL), columns], rhs[...])
            total = both[:, :LANES] + both[:, LANES:]
            if group:
                total += acc[ch, pl.ds(at, TALL), :]
            acc[ch, pl.ds(at, TALL), :] = total

        if count == 1:
            one(0)
        else:
            pl.loop(0, count)(one)

    def combine(ch, group):
        with jax.named_scope(f"load{ch}{group}"):
            ids = load(ch, group)
        with jax.named_scope(f"combine{ch}{group}"):
            tiles(ch, group, ids, jnp.int32(0), BLOCK_TILES // TALL)

    def combine_swap(ch, group):
        with jax.named_scope(f"load{ch}{group}"):
            ids = load(ch, group)
        copies = []
        with jax.named_scope(f"combine{ch}{group}"):
            tiles(ch, group, ids, theirs, HALF // TALL)
            for s in range(SUBS):
                at = pl.multiple_of(theirs + s * SUB, SUB)
                copies.append(
                    copy(acc.at[ch, pl.ds(at, SUB)], other.at[ch, s], d2s.at[ch, s], d2r.at[ch, s], partner)
                )
            tiles(ch, group, ids, mine, HALF // TALL)
        return copies

    def reduce_start(ch, s, swapped):
        with jax.named_scope(f"reduce{ch}{s}"):
            swapped.wait_recv()
            acc[ch, pl.ds(pl.multiple_of(mine + s * SUB, SUB), SUB), :] += other[ch, s]
            copies = []
            for k in (2, 1, 3):
                at = pl.multiple_of(mine + s * SUB + lax.rem(x + k, SIDE) * PIECE, PIECE)
                copies.append(
                    copy(
                        acc.at[ch, pl.ds(at, PIECE)], parts.at[ch, s, k - 1],
                        rss.at[ch, s, k - 1], rsr.at[ch, s, k - 1], pix_to(k),
                    )
                )
        return copies

    def gather_start(ch, s, copies):
        with jax.named_scope(f"gather{ch}{s}"):
            here = pl.multiple_of(mine + s * SUB + x * PIECE, PIECE)
            for c in copies:
                c.wait_recv()
            total = acc[ch, pl.ds(here, PIECE), :]
            for k in range(1, SIDE):
                total += parts[ch, s, k - 1]
            out[ch, pl.ds(here, PIECE), :] = total
            block = out.at[ch, pl.ds(here, PIECE)]
            gathers = [
                (k, copy(block, block, ags.at[ch, s, k - 1], agr.at[ch, s, k - 1], pix_to(k))) for k in (2, 1, 3)
            ]
        return gathers, [copy(block, block, fws.at[ch, s, 0], fwr.at[ch, s, 0], partner)]

    def forward(ch, s, started_gathers):
        gathers, sent = started_gathers
        with jax.named_scope(f"forward{ch}{s}"):
            for k, c in (gathers[1], gathers[2], gathers[0]):
                c.wait_recv()
                at = pl.multiple_of(mine + s * SUB + lax.rem(x - k + SIDE, SIDE) * PIECE, PIECE)
                block = out.at[ch, pl.ds(at, PIECE)]
                sent.append(copy(block, block, fws.at[ch, s, k], fwr.at[ch, s, k], partner))
        return sent

    for g in range(3):
        combine(0, g)
    s0 = combine_swap(0, 3)
    combine(1, 0)
    r0 = [reduce_start(0, s, s0[s]) for s in range(SUBS)]
    combine(1, 1)
    combine(1, 2)
    g0 = [gather_start(0, s, r0[s]) for s in range(SUBS)]
    s1 = combine_swap(1, 3)
    r1 = [reduce_start(1, s, s1[s]) for s in range(SUBS)]
    f0 = [forward(0, s, g0[s]) for s in range(SUBS)]
    g1 = [gather_start(1, s, r1[s]) for s in range(SUBS)]
    f1 = [forward(1, s, g1[s]) for s in range(SUBS)]
    with jax.named_scope("last"):
        for f in f0 + f1:
            for c in f:
                c.wait_recv()
        for c in started:
            c.wait_send()


def exchange(partial, keys, ids):
    vmem = pl.BlockSpec(memory_space=pltpu.VMEM)
    dma = pltpu.SemaphoreType.DMA
    return pl.pallas_call(
        exchange_kernel,
        out_shape=jax.ShapeDtypeStruct((2, BLOCK_TILES, LANES), F32),
        in_specs=[vmem] * 3,
        out_specs=vmem,
        scratch_shapes=[
            pltpu.VMEM((N_VOL, MSG, LANES), F32),
            pltpu.VMEM((N_VOL, MSG, LANES), F32),
            pltpu.VMEM((2, BLOCK_TILES, LANES), F32),
            pltpu.VMEM((2, SUBS, SUB, LANES), F32),
            pltpu.VMEM((2, SUBS, SIDE - 1, PIECE, LANES), F32),
            pltpu.VMEM((GROUP * CAP, 2 * LANES), BF16),
            pltpu.VMEM((BLOCK_TILES, N_VOL * CAP), BF16),
            pltpu.VMEM((N_VOL * CAP, SLOTS), BF16),
            dma((2, N_VOL)), dma((2, N_VOL)),
            dma((2, SUBS)), dma((2, SUBS)),
            dma((2, SUBS, SIDE - 1)), dma((2, SUBS, SIDE - 1)),
            dma((2, SUBS, SIDE - 1)), dma((2, SUBS, SIDE - 1)),
            dma((2, SUBS, SIDE)), dma((2, SUBS, SIDE)),
        ],
        compiler_params=pltpu.CompilerParams(
            collective_id=0, has_side_effects=True, vmem_limit_bytes=32 << 20
        ),
        name="exchange",
    )(partial, keys, ids)


def finish_kernel(map_ref, owner_ref, owned_ref, shell_h, rhs, sems):
    vol = lax.axis_index("vol")
    pix = lax.axis_index("pix")
    copies = []
    for ch in range(2):
        c = pltpu.make_async_copy(
            map_ref.at[ch], shell_h.at[:, pl.ds(ch * LANES, LANES)], sems.at[ch]
        )
        c.start()
        copies.append(c)
    rows = BLOCK_TILES // LANES
    owner = owner_ref[pl.ds(pl.multiple_of(vol * rows, rows), rows), :]
    match = (owner == pix).astype(F32).astype(BF16)
    before = (iota((LANES, LANES), 0) < iota((LANES, LANES), 1)).astype(F32).astype(BF16)
    above = (iota((rows, rows), 1) < iota((rows, rows), 0)).astype(F32).astype(BF16)
    ones = jnp.ones((LANES, LANES), BF16)
    rank = dot(match, before) + dot(dot(above, match).astype(BF16), ones)
    key = jnp.where(match.astype(F32) > 0, rank, -1.0)
    for ch in range(2):
        high, low = halves(map_ref[ch])
        rhs[:, ch * LANES : (ch + 1) * LANES] = high
        rhs[:, (ch + 2) * LANES : (ch + 3) * LANES] = low
    for t in range(OWN_MAX // BAND):
        place = (iota((BAND, LANES), 0) + t * BAND).astype(F32)
        chosen = jnp.concatenate(
            [(place == key[g : g + 1, :]).astype(F32).astype(BF16) for g in range(rows)], 1
        )
        both = dot(chosen, rhs[...])
        owned_ref[t * BAND : (t + 1) * BAND, :] = both[:, : 2 * LANES] + both[:, 2 * LANES :]
    for c in copies:
        c.wait()


def finish(block_map, tile_owner):
    vmem = pl.BlockSpec(memory_space=pltpu.VMEM)
    return pl.pallas_call(
        finish_kernel,
        out_shape=(
            jax.ShapeDtypeStruct((OWN_MAX, 2 * LANES), F32),
            jax.ShapeDtypeStruct((BLOCK_TILES, 2 * LANES), F32),
        ),
        in_specs=[vmem, vmem],
        out_specs=(vmem, pl.BlockSpec(memory_space=pltpu.HBM)),
        scratch_shapes=[pltpu.VMEM((BLOCK_TILES, 4 * LANES), BF16), pltpu.SemaphoreType.DMA((2,))],
        compiler_params=pltpu.CompilerParams(vmem_limit_bytes=16 << 20),
        name="finish",
    )(block_map, tile_owner)


def shards(kernel, pressure, velocity, entry_slot, slot_tile, tile_owner):
    square = (ENTRIES // LANES, LANES)
    partial, keys, ids = project(
        kernel,
        pressure.reshape(square),
        velocity.reshape(square),
        entry_slot.reshape(square),
        slot_tile.reshape(SLOTS // LANES, LANES),
    )
    block_map = exchange(partial, keys, ids)
    return finish(block_map, tile_owner.reshape(-1, LANES))


def solution(mesh):
    in_specs = (
        P(("vol", "pix"), None),
        P(("vol", "pix")),
        P(("vol", "pix")),
        P(("vol", "pix"), None),
        P(("vol", "pix"), None),
        P(),
    )
    out_specs = (P(("vol", "pix"), None), P("vol", None))
    return jax.shard_map(shards, mesh=mesh, in_specs=in_specs, out_specs=out_specs, check_vma=False)
```

```python
import functools

import jax
import jax.numpy as jnp
from jax import lax
from jax.experimental import pallas as pl
from jax.experimental.pallas import tpu as pltpu
from jax.sharding import PartitionSpec as P

MESH = pl.DeviceIdType.MESH
F32 = jnp.float32
BF16 = jnp.bfloat16

LANES = 128
ENTRIES = 16384
SLOTS = 1024
N_VOL = 16
SIDE = 4
BLOCK_TILES = 2048
CAP = 128
OWN_MAX = 512

STEP = 2048
SPAN = 256
WINDOW = 32
MSG = 2 * CAP + 8
FIRST = CAP + 8


def dot(a, b):
    return jnp.dot(a, b, preferred_element_type=F32)


def iota(shape, dim):
    return lax.broadcasted_iota(jnp.int32, shape, dim)


def halves(x):
    high = x.astype(BF16)
    return high, (x - high.astype(F32)).astype(BF16)


def equal(place, row):
    return jnp.where(place == row, jnp.ones((), BF16), jnp.zeros((), BF16))


def project_kernel(
    kernel_h, pressure_h, velocity_h, slot_h, tile_h, rhs_ref, pick_ref, ids_ref,
    weights, pressure, velocity, slot_v, tile_v, slot_s, acc, sems, chunk_sems,
):
    steps = ENTRIES // STEP
    rows = STEP // LANES
    small = [
        pltpu.make_async_copy(a, b, sems.at[n])
        for n, (a, b) in enumerate(
            (
                (tile_h, tile_v), (slot_h, slot_s), (slot_h, slot_v),
                (pressure_h, pressure), (velocity_h, velocity),
            )
        )
    ]
    for c in small:
        c.start()

    def chunk(g):
        span = pl.ds(pl.multiple_of(g * STEP, STEP), STEP)
        return pltpu.make_async_copy(kernel_h.at[span], weights.at[span], chunk_sems.at[g])

    for g in range(steps):
        chunk(g).start()
    acc[...] = jnp.zeros_like(acc)

    small[0].wait()
    tiles = tile_v[...]
    block = tiles // BLOCK_TILES
    within = tiles - block * BLOCK_TILES
    groups = SLOTS // LANES
    match = jnp.concatenate([(block == v).astype(F32) for v in range(N_VOL)], 0)
    r, c = iota((LANES, LANES), 0), iota((LANES, LANES), 1)
    before = (r < c).astype(F32).astype(BF16)
    above = ((c < r) & (c // groups == r // groups)).astype(F32).astype(BF16)
    ones = jnp.ones((LANES, LANES), BF16)
    packed = match.astype(BF16)
    rank = dot(packed, before) + dot(dot(above, packed).astype(BF16), ones)
    key = jnp.where(match > 0, rank, -1.0).astype(BF16)
    own = jnp.zeros((groups, LANES), F32)
    for v in range(N_VOL):
        own += match[v * groups : (v + 1) * groups] * rank[v * groups : (v + 1) * groups]
    place = iota((LANES, LANES), 0).astype(F32).astype(BF16)
    spread = jnp.concatenate([equal(place, own[g : g + 1].astype(BF16)) for g in range(groups)], 1)
    for v in range(N_VOL):
        for g in range(groups):
            row = v * groups + g
            pick_ref[v * CAP : (v + 1) * CAP, g * LANES : (g + 1) * LANES] = equal(place, key[row : row + 1])
    vols = iota((N_VOL, LANES), 0)
    upper, lower = (within // 64).astype(F32), (within % 64).astype(F32)
    table = []
    for values in (upper, lower, jnp.ones_like(upper)):
        table.append(
            jnp.concatenate(
                [jnp.where(vols == block[g : g + 1], values[g : g + 1], 0.0) for g in range(groups)], 1
            )
        )
    table = jnp.concatenate(table, 0).astype(BF16)
    found = lax.dot_general(table, spread, (((1,), (1,)), ((), ())), preferred_element_type=F32)
    ids_ref[...] = found[:N_VOL] * 64.0 + found[N_VOL : 2 * N_VOL] + found[2 * N_VOL :] - 1.0

    for n in (1, 2, 3, 4):
        small[n].wait()
    lines = iota((WINDOW, LANES), 0)
    per = SPAN // LANES

    @pl.loop(0, steps)
    def _(g):
        chunk(g).wait()
        top = pl.multiple_of(g * rows, rows)
        thermal = pressure[pl.ds(top, rows), :].astype(F32)
        kinetic = velocity[pl.ds(top, rows), :].astype(F32)
        slots = slot_v[pl.ds(top, rows), :]

        def products(i, base):
            up, low = [], []
            for h in range(per):
                n = i * per + h
                match = lines == slots[n : n + 1, :] - base
                up.append(jnp.where(match, thermal[n : n + 1, :], 0.0))
                low.append(jnp.where(match, kinetic[n : n + 1, :], 0.0))
            amplitudes = jnp.concatenate([jnp.concatenate(up, 1), jnp.concatenate(low, 1)], 0)
            span = pl.ds(pl.multiple_of(g * STEP + i * SPAN, SPAN), SPAN)
            return dot(amplitudes.astype(BF16), weights[span, :])

        def add(base, value):
            acc[0, pl.ds(base, WINDOW), :] += value[:WINDOW]
            acc[1, pl.ds(base, WINDOW), :] += value[WINDOW:]

        count = STEP // SPAN
        bases, lasts = [], []
        for i in range(count):
            bases.append(pl.multiple_of(slot_s[top + i * per, 0] & -8, 8))
            lasts.append(slot_s[top + i * per + per - 1, LANES - 1])
        values = [products(i, bases[i]) for i in range(count)]
        for i in range(count):
            add(bases[i], values[i])
        widest = lasts[0] - bases[0]
        for i in range(1, count):
            widest = jnp.maximum(widest, lasts[i] - bases[i])

        @pl.when(widest >= WINDOW)
        def _():
            for i in range(count):

                @pl.loop(1, (lasts[i] - bases[i]) // WINDOW + 1)
                def _(w, i=i):
                    base = pl.multiple_of(bases[i] + w * WINDOW, 8)
                    add(base, products(i, base))

    for ch in range(2):
        high, low = halves(acc[ch, :SLOTS, :])
        rhs_ref[:, 2 * ch * LANES : (2 * ch + 1) * LANES] = high
        rhs_ref[:, (2 * ch + 1) * LANES : (2 * ch + 2) * LANES] = low


def project(kernel, pressure, velocity, entry_slot, slot_tile):
    outs = (((SLOTS, 4 * LANES), BF16), ((N_VOL * CAP, SLOTS), BF16), ((N_VOL, LANES), F32))
    square = (ENTRIES // LANES, LANES)
    return pl.pallas_call(
        project_kernel,
        out_shape=tuple(jax.ShapeDtypeStruct(*o) for o in outs),
        in_specs=[pl.BlockSpec(memory_space=pltpu.HBM)] * 5,
        out_specs=tuple(pl.BlockSpec(memory_space=pltpu.VMEM) for o in outs),
        scratch_shapes=[
            pltpu.VMEM((ENTRIES, LANES), BF16),
            pltpu.VMEM(square, BF16),
            pltpu.VMEM(square, BF16),
            pltpu.VMEM(square, jnp.int32),
            pltpu.VMEM((SLOTS // LANES, LANES), jnp.int32),
            pltpu.SMEM(square, jnp.int32),
            pltpu.VMEM((2, SLOTS + WINDOW + 8, LANES), F32),
            pltpu.SemaphoreType.DMA((5,)),
            pltpu.SemaphoreType.DMA((ENTRIES // STEP,)),
        ],
        compiler_params=pltpu.CompilerParams(vmem_limit_bytes=16 << 20),
        name="project",
    )(*(pltpu.with_memory_space_constraint(a, pltpu.HBM) for a in (kernel, pressure, velocity, entry_slot, slot_tile)))


GROUP = 4
SUBS = 2
HALF = BLOCK_TILES // 2
SUB = HALF // SUBS
PIECE = SUB // SIDE
TALL = 1024
BAND = 256
ORDER = (0, 1, 4, 3, 12, 5, 15, 7, 13, 2, 8, 6, 9, 10, 14, 11)
ROUND = 4


def exchange_kernel(
    partial, pick, ids_ref, out, send, recv, acc, other, parts, rhs, hot,
    p1s, p1r, d2s, d2r, rss, rsr, ags, agr, fws, fwr,
):
    vol = lax.axis_index("vol")
    pix = lax.axis_index("pix")
    x, core = pix // 2, pix % 2
    y, z = vol // SIDE, vol % SIDE

    def vol_to(k):
        return lax.rem(y + k // SIDE, SIDE) * SIDE + lax.rem(z + k % SIDE, SIDE)

    def pix_to(k):
        return {"pix": lax.rem(x + k, SIDE) * 2 + core}

    partner = {"pix": x * 2 + 1 - core}
    peers = [{"vol": vol_to(k)} for k in range(1, N_VOL)] + [pix_to(k) for k in range(1, SIDE)] + [partner]
    barrier = pltpu.get_barrier_semaphore()
    for peer in peers:
        pl.semaphore_signal(barrier, inc=1, device_id=peer, device_id_type=MESH)

    def remote(src, dst, s, r, peer):
        return pltpu.make_async_remote_copy(
            src_ref=src, dst_ref=dst, send_sem=s, recv_sem=r, device_id=peer, device_id_type=MESH
        )

    def copy(src, dst, s, r, peer):
        c = remote(src, dst, s, r, peer)
        c.start()
        return c

    spans = ((0, FIRST), (FIRST, CAP))
    rows_of = (0, FIRST)
    def launch(ch, n):
        begin, size = spans[ch]
        copy(
            send.at[n, pl.ds(begin, size)],
            recv.at[n, pl.ds(begin, size)],
            p1s.at[0], p1r.at[ch, n // GROUP], {"vol": vol_to(ORDER[n])},
        )

    def arrived(ch, group):
        begin, size = spans[ch]
        low = max(group * GROUP, 1)
        span = pl.ds(low, (group + 1) * GROUP - low)
        span = recv.at[span, pl.ds(begin, size)]
        remote(span, span, p1s.at[0], p1r.at[ch, group], partner).wait_recv()

    def batch(ch, ns):
        rows = []
        for n in ns:
            to = vol_to(ORDER[n])
            rows.append(pick[pl.ds(pl.multiple_of(to * CAP, CAP), CAP), :])
            if ch == 0:
                send[n, CAP:FIRST, :] = jnp.broadcast_to(ids_ref[pl.ds(to, 1), :], (8, LANES))
        both = dot(jnp.concatenate(rows, 0), partial[:, 2 * ch * LANES : 2 * (ch + 1) * LANES])
        total = both[:, :LANES] + both[:, LANES:]
        for m, n in enumerate(ns):
            send[n, rows_of[ch] : rows_of[ch] + CAP, :] = total[m * CAP : (m + 1) * CAP]

    todo = tuple(range(1, N_VOL)) + (0,)
    waiting = []
    with jax.named_scope("messages"):
        for ch in range(2):
            for n in range(0, N_VOL, ROUND):
                ns = todo[n : n + ROUND]
                batch(ch, ns)
                if ch == 0 and n == 0:
                    pl.semaphore_wait(barrier, len(peers))
                for c, m in waiting:
                    launch(c, m)
                waiting = [(ch, m) for m in ns if m]
        for c, m in waiting:
            launch(c, m)

    band = iota((BAND, LANES), 0).astype(F32).astype(BF16)
    mine = core * HALF
    theirs = HALF - mine
    turn = GROUP * CAP

    def load(ch, group):
        ids = []
        arrived(ch, group)
        for n in range(GROUP):
            k = group * GROUP + n
            source = recv if k else send
            ids.append(source[k, CAP : CAP + 1, :])
            high, low = halves(source[k, rows_of[ch] : rows_of[ch] + CAP, :])
            rhs[n * CAP : (n + 1) * CAP, :LANES] = high
            rhs[n * CAP : (n + 1) * CAP, LANES:] = low
        return ids

    def tiles(ch, group, ids, begin, count):
        columns = slice(group * turn, (group + 1) * turn)

        def one(t):
            at = pl.multiple_of(begin + t * TALL, TALL)
            if ch == 0:
                for b in range(TALL // BAND):
                    low = pl.multiple_of(at + b * BAND, BAND)
                    pieces = []
                    for i in ids:
                        local = i - low.astype(F32)
                        local = jnp.where((local >= 0) & (local < BAND), local, -1.0)
                        pieces.append(equal(band, local.astype(BF16)))
                    hot[pl.ds(low, BAND), columns] = jnp.concatenate(pieces, 1)
            both = dot(hot[pl.ds(at, TALL), columns], rhs[...])
            total = both[:, :LANES] + both[:, LANES:]
            if group:
                total += acc[ch, pl.ds(at, TALL), :]
            acc[ch, pl.ds(at, TALL), :] = total

        if count == 1:
            one(0)
        else:
            pl.loop(0, count)(one)

    def combine(ch, group):
        with jax.named_scope(f"load{ch}{group}"):
            ids = load(ch, group)
        with jax.named_scope(f"combine{ch}{group}"):
            tiles(ch, group, ids, jnp.int32(0), BLOCK_TILES // TALL)

    def combine_swap(ch, group):
        with jax.named_scope(f"load{ch}{group}"):
            ids = load(ch, group)
        copies = []
        with jax.named_scope(f"combine{ch}{group}"):
            tiles(ch, group, ids, theirs, HALF // TALL)
            for s in range(SUBS):
                at = pl.multiple_of(theirs + s * SUB, SUB)
                copies.append(
                    copy(acc.at[ch, pl.ds(at, SUB)], other.at[ch, s], d2s.at[0], d2r.at[ch, s], partner)
                )
            tiles(ch, group, ids, mine, HALF // TALL)
        return copies

    def reduce_start(ch, s, swapped):
        with jax.named_scope(f"reduce{ch}{s}"):
            swapped.wait_recv()
            acc[ch, pl.ds(pl.multiple_of(mine + s * SUB, SUB), SUB), :] += other[ch, s]
            copies = []
            for k in (2, 1, 3):
                at = pl.multiple_of(mine + s * SUB + lax.rem(x + k, SIDE) * PIECE, PIECE)
                copies.append(
                    copy(
                        acc.at[ch, pl.ds(at, PIECE)], parts.at[ch, s, k - 1],
                        rss.at[0], rsr.at[ch, s], pix_to(k),
                    )
                )
        return copies

    def gather_start(ch, s, copies):
        with jax.named_scope(f"gather{ch}{s}"):
            here = pl.multiple_of(mine + s * SUB + x * PIECE, PIECE)
            remote(parts.at[ch, s], parts.at[ch, s], rss.at[0], rsr.at[ch, s], partner).wait_recv()
            total = acc[ch, pl.ds(here, PIECE), :]
            for k in range(1, SIDE):
                total += parts[ch, s, k - 1]
            out[ch, pl.ds(here, PIECE), :] = total
            block = out.at[ch, pl.ds(here, PIECE)]
            gathers = [
                (k, copy(block, block, ags.at[0], agr.at[ch, s, k - 1], pix_to(k))) for k in (2, 1, 3)
            ]
        return gathers, [copy(block, block, fws.at[0], fwr.at[ch], partner)]

    def forward(ch, s, started_gathers):
        gathers, sent = started_gathers
        with jax.named_scope(f"forward{ch}{s}"):
            for k, c in (gathers[1], gathers[2], gathers[0]):
                c.wait_recv()
                at = pl.multiple_of(mine + s * SUB + lax.rem(x - k + SIDE, SIDE) * PIECE, PIECE)
                block = out.at[ch, pl.ds(at, PIECE)]
                copy(block, block, fws.at[0], fwr.at[ch], partner)
        return sent

    for g in range(3):
        combine(0, g)
    s0 = combine_swap(0, 3)
    r0 = [reduce_start(0, s, s0[s]) for s in range(SUBS)]
    combine(1, 0)
    combine(1, 1)
    combine(1, 2)
    g0 = [gather_start(0, s, r0[s]) for s in range(SUBS)]
    s1 = combine_swap(1, 3)
    r1 = [reduce_start(1, s, s1[s]) for s in range(SUBS)]
    f0 = [forward(0, s, g0[s]) for s in range(SUBS)]
    g1 = [gather_start(1, s, r1[s]) for s in range(SUBS)]
    f1 = [forward(1, s, g1[s]) for s in range(SUBS)]
    with jax.named_scope("last"):
        for ch in range(2):
            block = out.at[ch, pl.ds(pl.multiple_of(theirs, HALF), HALF)]
            remote(block, block, fws.at[0], fwr.at[ch], partner).wait_recv()
        for whole, sem in (
            (send.at[pl.ds(1, N_VOL - 1)], p1s),
            (other, d2s),
            (parts, rss),
            (parts, ags),
            (out.at[:, pl.ds(0, HALF)], fws),
        ):
            remote(whole, whole, sem.at[0], d2r.at[0, 0], partner).wait_send()


def exchange(partial, pick, ids):
    vmem = pl.BlockSpec(memory_space=pltpu.VMEM)
    dma = pltpu.SemaphoreType.DMA
    return pl.pallas_call(
        exchange_kernel,
        out_shape=jax.ShapeDtypeStruct((2, BLOCK_TILES, LANES), F32),
        in_specs=[vmem] * 3,
        out_specs=vmem,
        scratch_shapes=[
            pltpu.VMEM((N_VOL, MSG, LANES), F32),
            pltpu.VMEM((N_VOL, MSG, LANES), F32),
            pltpu.VMEM((2, BLOCK_TILES, LANES), F32),
            pltpu.VMEM((2, SUBS, SUB, LANES), F32),
            pltpu.VMEM((2, SUBS, SIDE - 1, PIECE, LANES), F32),
            pltpu.VMEM((GROUP * CAP, 2 * LANES), BF16),
            pltpu.VMEM((BLOCK_TILES, N_VOL * CAP), BF16),
            dma((1,)), dma((2, N_VOL // GROUP)),
            dma((1,)), dma((2, SUBS)),
            dma((1,)), dma((2, SUBS)),
            dma((1,)), dma((2, SUBS, SIDE - 1)),
            dma((1,)), dma((2,)),
        ],
        compiler_params=pltpu.CompilerParams(
            collective_id=0, has_side_effects=True, vmem_limit_bytes=32 << 20
        ),
        name="exchange",
    )(partial, pick, ids)


def finish_kernel(map_ref, owner_ref, owned_h, shell_h, owned, rhs, sems):
    vol = lax.axis_index("vol")
    pix = lax.axis_index("pix")
    copies = []
    for ch in range(2):
        c = pltpu.make_async_copy(
            map_ref.at[ch], shell_h.at[:, pl.ds(ch * LANES, LANES)], sems.at[ch]
        )
        c.start()
        copies.append(c)
    rows = BLOCK_TILES // LANES
    owner = owner_ref[pl.ds(pl.multiple_of(vol * rows, rows), rows), :]
    match = (owner == pix).astype(F32).astype(BF16)
    before = (iota((LANES, LANES), 0) < iota((LANES, LANES), 1)).astype(F32).astype(BF16)
    above = (iota((rows, rows), 1) < iota((rows, rows), 0)).astype(F32).astype(BF16)
    ones = jnp.ones((LANES, LANES), BF16)
    rank = dot(match, before) + dot(dot(above, match).astype(BF16), ones)
    key = jnp.where(match.astype(F32) > 0, rank, -1.0)
    for ch in range(2):
        high, low = halves(map_ref[ch])
        rhs[:, ch * LANES : (ch + 1) * LANES] = high
        rhs[:, (ch + 2) * LANES : (ch + 3) * LANES] = low
    place = iota((BAND, LANES), 0).astype(F32).astype(BF16)
    for t in range(OWN_MAX // BAND):
        local = key - t * BAND
        local = jnp.where((local >= 0) & (local < BAND), local, -1.0).astype(BF16)
        chosen = jnp.concatenate([equal(place, local[g : g + 1]) for g in range(rows)], 1)
        both = dot(chosen, rhs[...])
        here = pl.ds(t * BAND, BAND)
        owned[here, :] = both[:, : 2 * LANES] + both[:, 2 * LANES :]
        c = pltpu.make_async_copy(owned.at[here], owned_h.at[here], sems.at[2 + t])
        c.start()
        copies.append(c)
    for c in copies:
        c.wait()


def finish(block_map, tile_owner):
    vmem = pl.BlockSpec(memory_space=pltpu.VMEM)
    return pl.pallas_call(
        finish_kernel,
        out_shape=(
            jax.ShapeDtypeStruct((OWN_MAX, 2 * LANES), F32),
            jax.ShapeDtypeStruct((BLOCK_TILES, 2 * LANES), F32),
        ),
        in_specs=[vmem, vmem],
        out_specs=(pl.BlockSpec(memory_space=pltpu.HBM),) * 2,
        scratch_shapes=[
            pltpu.VMEM((OWN_MAX, 2 * LANES), F32),
            pltpu.VMEM((BLOCK_TILES, 4 * LANES), BF16),
            pltpu.SemaphoreType.DMA((2 + OWN_MAX // BAND,)),
        ],
        compiler_params=pltpu.CompilerParams(vmem_limit_bytes=16 << 20),
        name="finish",
    )(block_map, tile_owner)


def shards(kernel, pressure, velocity, entry_slot, slot_tile, tile_owner):
    square = (ENTRIES // LANES, LANES)
    partial, pick, ids = project(
        kernel,
        pressure.reshape(square),
        velocity.reshape(square),
        entry_slot.reshape(square),
        slot_tile.reshape(SLOTS // LANES, LANES),
    )
    block_map = exchange(partial, pick, ids)
    return finish(block_map, tile_owner.reshape(-1, LANES))


def solution(mesh):
    in_specs = (
        P(("vol", "pix"), None),
        P(("vol", "pix")),
        P(("vol", "pix")),
        P(("vol", "pix"), None),
        P(("vol", "pix"), None),
        P(),
    )
    out_specs = (P(("vol", "pix"), None), P("vol", None))
    return jax.shard_map(shards, mesh=mesh, in_specs=in_specs, out_specs=out_specs, check_vma=False)
```

```python
import functools

import jax
import jax.numpy as jnp
from jax import lax
from jax.experimental import pallas as pl
from jax.experimental.pallas import tpu as pltpu
from jax.sharding import PartitionSpec as P

MESH = pl.DeviceIdType.MESH
F32 = jnp.float32
BF16 = jnp.bfloat16

LANES = 128
ENTRIES = 16384
SLOTS = 1024
N_VOL = 16
SIDE = 4
BLOCK_TILES = 2048
CAP = 128
OWN_MAX = 512

STEP = 2048
SPAN = 256
WINDOW = 32
MSG = 2 * CAP + 8
FIRST = CAP + 8


def dot(a, b):
    return jnp.dot(a, b, preferred_element_type=F32)


def iota(shape, dim):
    return lax.broadcasted_iota(jnp.int32, shape, dim)


def halves(x):
    high = x.astype(BF16)
    return high, (x - high.astype(F32)).astype(BF16)


def equal(place, row):
    return jnp.where(place == row, jnp.ones((), BF16), jnp.zeros((), BF16))


def project_kernel(
    kernel_h, pressure_h, velocity_h, slot_h, tile_h, rhs_ref, pick_ref, ids_ref,
    weights, pressure, velocity, slot_v, tile_v, slot_s, acc, sems, chunk_sems,
):
    steps = ENTRIES // STEP
    rows = STEP // LANES
    small = [
        pltpu.make_async_copy(a, b, sems.at[n])
        for n, (a, b) in enumerate(
            (
                (tile_h, tile_v), (slot_h, slot_s), (slot_h, slot_v),
                (pressure_h, pressure), (velocity_h, velocity),
            )
        )
    ]
    for c in small:
        c.start()

    def chunk(g):
        span = pl.ds(pl.multiple_of(g * STEP, STEP), STEP)
        return pltpu.make_async_copy(kernel_h.at[span], weights.at[span], chunk_sems.at[g])

    for g in range(steps):
        chunk(g).start()
    acc[...] = jnp.zeros_like(acc)

    small[0].wait()
    tiles = tile_v[...]
    block = tiles // BLOCK_TILES
    within = tiles - block * BLOCK_TILES
    groups = SLOTS // LANES
    match = jnp.concatenate([(block == v).astype(F32) for v in range(N_VOL)], 0)
    r, c = iota((LANES, LANES), 0), iota((LANES, LANES), 1)
    before = (r < c).astype(F32).astype(BF16)
    above = ((c < r) & (c // groups == r // groups)).astype(F32).astype(BF16)
    ones = jnp.ones((LANES, LANES), BF16)
    packed = match.astype(BF16)
    rank = dot(packed, before) + dot(dot(above, packed).astype(BF16), ones)
    key = jnp.where(match > 0, rank, -1.0).astype(BF16)
    own = jnp.zeros((groups, LANES), F32)
    for v in range(N_VOL):
        own += match[v * groups : (v + 1) * groups] * rank[v * groups : (v + 1) * groups]
    place = iota((LANES, LANES), 0).astype(F32).astype(BF16)
    spread = jnp.concatenate([equal(place, own[g : g + 1].astype(BF16)) for g in range(groups)], 1)
    for v in range(N_VOL):
        for g in range(groups):
            row = v * groups + g
            pick_ref[v * CAP : (v + 1) * CAP, g * LANES : (g + 1) * LANES] = equal(place, key[row : row + 1])
    vols = iota((N_VOL, LANES), 0)
    upper, lower = (within // 64).astype(F32), (within % 64).astype(F32)
    table = []
    for values in (upper, lower, jnp.ones_like(upper)):
        table.append(
            jnp.concatenate(
                [jnp.where(vols == block[g : g + 1], values[g : g + 1], 0.0) for g in range(groups)], 1
            )
        )
    table = jnp.concatenate(table, 0).astype(BF16)
    found = lax.dot_general(table, spread, (((1,), (1,)), ((), ())), preferred_element_type=F32)
    ids_ref[...] = found[:N_VOL] * 64.0 + found[N_VOL : 2 * N_VOL] + found[2 * N_VOL :] - 1.0

    for n in (1, 2, 3, 4):
        small[n].wait()
    lines = iota((WINDOW, LANES), 0)
    per = SPAN // LANES

    @pl.loop(0, steps)
    def _(g):
        chunk(g).wait()
        top = pl.multiple_of(g * rows, rows)
        thermal = pressure[pl.ds(top, rows), :].astype(F32)
        kinetic = velocity[pl.ds(top, rows), :].astype(F32)
        slots = slot_v[pl.ds(top, rows), :]

        def products(i, base):
            up, low = [], []
            for h in range(per):
                n = i * per + h
                match = lines == slots[n : n + 1, :] - base
                up.append(jnp.where(match, thermal[n : n + 1, :], 0.0))
                low.append(jnp.where(match, kinetic[n : n + 1, :], 0.0))
            amplitudes = jnp.concatenate([jnp.concatenate(up, 1), jnp.concatenate(low, 1)], 0)
            span = pl.ds(pl.multiple_of(g * STEP + i * SPAN, SPAN), SPAN)
            return dot(amplitudes.astype(BF16), weights[span, :])

        def add(base, value):
            acc[0, pl.ds(base, WINDOW), :] += value[:WINDOW]
            acc[1, pl.ds(base, WINDOW), :] += value[WINDOW:]

        count = STEP // SPAN
        bases, lasts = [], []
        for i in range(count):
            bases.append(pl.multiple_of(slot_s[top + i * per, 0] & -8, 8))
            lasts.append(slot_s[top + i * per + per - 1, LANES - 1])
        values = [products(i, bases[i]) for i in range(count)]
        for i in range(count):
            add(bases[i], values[i])
        widest = lasts[0] - bases[0]
        for i in range(1, count):
            widest = jnp.maximum(widest, lasts[i] - bases[i])

        @pl.when(widest >= WINDOW)
        def _():
            for i in range(count):

                @pl.loop(1, (lasts[i] - bases[i]) // WINDOW + 1)
                def _(w, i=i):
                    base = pl.multiple_of(bases[i] + w * WINDOW, 8)
                    add(base, products(i, base))

    for ch in range(2):
        high, low = halves(acc[ch, :SLOTS, :])
        rhs_ref[:, 2 * ch * LANES : (2 * ch + 1) * LANES] = high
        rhs_ref[:, (2 * ch + 1) * LANES : (2 * ch + 2) * LANES] = low


def project(kernel, pressure, velocity, entry_slot, slot_tile):
    outs = (((SLOTS, 4 * LANES), BF16), ((N_VOL * CAP, SLOTS), BF16), ((N_VOL, LANES), F32))
    square = (ENTRIES // LANES, LANES)
    return pl.pallas_call(
        project_kernel,
        out_shape=tuple(jax.ShapeDtypeStruct(*o) for o in outs),
        in_specs=[pl.BlockSpec(memory_space=pltpu.HBM)] * 5,
        out_specs=tuple(pl.BlockSpec(memory_space=pltpu.VMEM) for o in outs),
        scratch_shapes=[
            pltpu.VMEM((ENTRIES, LANES), BF16),
            pltpu.VMEM(square, BF16),
            pltpu.VMEM(square, BF16),
            pltpu.VMEM(square, jnp.int32),
            pltpu.VMEM((SLOTS // LANES, LANES), jnp.int32),
            pltpu.SMEM(square, jnp.int32),
            pltpu.VMEM((2, SLOTS + WINDOW + 8, LANES), F32),
            pltpu.SemaphoreType.DMA((5,)),
            pltpu.SemaphoreType.DMA((ENTRIES // STEP,)),
        ],
        compiler_params=pltpu.CompilerParams(vmem_limit_bytes=16 << 20),
        name="project",
    )(*(pltpu.with_memory_space_constraint(a, pltpu.HBM) for a in (kernel, pressure, velocity, entry_slot, slot_tile)))


GROUP = 4
SUBS = 2
HALF = BLOCK_TILES // 2
SUB = HALF // SUBS
PIECE = SUB // SIDE
TALL = 1024
BAND = 256
ORDER = (0, 4, 12, 1, 3, 8, 2, 5, 7, 13, 15, 9, 11, 6, 14, 10)
ROUND = 16


def exchange_kernel(
    partial, pick, ids_ref, out, send, recv, acc, other, parts, rhs, hot,
    p1s, p1r, d2s, d2r, rss, rsr, ags, agr, fws, fwr,
):
    vol = lax.axis_index("vol")
    pix = lax.axis_index("pix")
    x, core = pix // 2, pix % 2
    y, z = vol // SIDE, vol % SIDE

    def vol_to(k):
        return lax.rem(y + k // SIDE, SIDE) * SIDE + lax.rem(z + k % SIDE, SIDE)

    def pix_to(k):
        return {"pix": lax.rem(x + k, SIDE) * 2 + core}

    partner = {"pix": x * 2 + 1 - core}
    peers = [{"vol": vol_to(k)} for k in range(1, N_VOL)] + [pix_to(k) for k in range(1, SIDE)] + [partner]
    barrier = pltpu.get_barrier_semaphore()
    for peer in peers:
        pl.semaphore_signal(barrier, inc=1, device_id=peer, device_id_type=MESH)

    def remote(src, dst, s, r, peer):
        return pltpu.make_async_remote_copy(
            src_ref=src, dst_ref=dst, send_sem=s, recv_sem=r, device_id=peer, device_id_type=MESH
        )

    def copy(src, dst, s, r, peer):
        c = remote(src, dst, s, r, peer)
        c.start()
        return c

    spans = ((0, CAP + 1), (FIRST, CAP))
    rows_of = (0, FIRST)
    def launch(ch, n):
        begin, size = spans[ch]
        copy(
            send.at[n, pl.ds(begin, size)],
            recv.at[n, pl.ds(begin, size)],
            p1s.at[0], p1r.at[ch, n // GROUP], {"vol": vol_to(ORDER[n])},
        )

    def arrived(ch, group):
        begin, size = spans[ch]
        low = max(group * GROUP, 1)
        span = pl.ds(low, (group + 1) * GROUP - low)
        span = recv.at[span, pl.ds(begin, size)]
        remote(span, span, p1s.at[0], p1r.at[ch, group], partner).wait_recv()

    def batch(ch, ns):
        rows = []
        for n in ns:
            to = vol_to(ORDER[n])
            rows.append(pick[pl.ds(pl.multiple_of(to * CAP, CAP), CAP), :])
            if ch == 0:
                send[n, CAP:FIRST, :] = jnp.broadcast_to(ids_ref[pl.ds(to, 1), :], (8, LANES))
        both = dot(jnp.concatenate(rows, 0), partial[:, 2 * ch * LANES : 2 * (ch + 1) * LANES])
        total = both[:, :LANES] + both[:, LANES:]
        for m, n in enumerate(ns):
            send[n, rows_of[ch] : rows_of[ch] + CAP, :] = total[m * CAP : (m + 1) * CAP]

    todo = tuple(range(1, N_VOL)) + (0,)
    with jax.named_scope("messages"):
        for n in range(0, N_VOL, ROUND):
            batch(0, todo[n : n + ROUND])
        pl.semaphore_wait(barrier, len(peers))
        for n in range(1, N_VOL):
            launch(0, n)
        for n in range(0, N_VOL, ROUND):
            batch(1, todo[n : n + ROUND])

    def launch_second():
        for n in range(1, N_VOL):
            launch(1, n)

    band = iota((BAND, LANES), 0).astype(F32).astype(BF16)
    mine = core * HALF
    theirs = HALF - mine
    turn = GROUP * CAP

    def load(ch, group):
        ids = []
        arrived(ch, group)
        if ch == 0 and group == 1:
            launch_second()
        for n in range(GROUP):
            k = group * GROUP + n
            source = recv if k else send
            ids.append(source[k, CAP : CAP + 1, :])
            high, low = halves(source[k, rows_of[ch] : rows_of[ch] + CAP, :])
            rhs[n * CAP : (n + 1) * CAP, :LANES] = high
            rhs[n * CAP : (n + 1) * CAP, LANES:] = low
        return ids

    def tiles(ch, group, ids, begin, count):
        columns = slice(group * turn, (group + 1) * turn)

        def one(t):
            at = pl.multiple_of(begin + t * TALL, TALL)
            if ch == 0:
                for b in range(TALL // BAND):
                    low = pl.multiple_of(at + b * BAND, BAND)
                    pieces = []
                    for i in ids:
                        local = i - low.astype(F32)
                        local = jnp.where((local >= 0) & (local < BAND), local, -1.0)
                        pieces.append(equal(band, local.astype(BF16)))
                    hot[pl.ds(low, BAND), columns] = jnp.concatenate(pieces, 1)
            both = dot(hot[pl.ds(at, TALL), columns], rhs[...])
            total = both[:, :LANES] + both[:, LANES:]
            if group:
                total += acc[ch, pl.ds(at, TALL), :]
            acc[ch, pl.ds(at, TALL), :] = total

        if count == 1:
            one(0)
        else:
            pl.loop(0, count)(one)

    def combine(ch, group):
        with jax.named_scope(f"load{ch}{group}"):
            ids = load(ch, group)
        with jax.named_scope(f"combine{ch}{group}"):
            tiles(ch, group, ids, jnp.int32(0), BLOCK_TILES // TALL)

    def combine_swap(ch, group):
        with jax.named_scope(f"load{ch}{group}"):
            ids = load(ch, group)
        copies = []
        with jax.named_scope(f"combine{ch}{group}"):
            tiles(ch, group, ids, theirs, HALF // TALL)
            for s in range(SUBS):
                at = pl.multiple_of(theirs + s * SUB, SUB)
                copies.append(
                    copy(acc.at[ch, pl.ds(at, SUB)], other.at[ch, s], d2s.at[0], d2r.at[ch, s], partner)
                )
            tiles(ch, group, ids, mine, HALF // TALL)
        return copies

    def reduce_start(ch, s, swapped):
        with jax.named_scope(f"reduce{ch}{s}"):
            swapped.wait_recv()
            acc[ch, pl.ds(pl.multiple_of(mine + s * SUB, SUB), SUB), :] += other[ch, s]
            copies = []
            for k in (2, 1, 3):
                at = pl.multiple_of(mine + s * SUB + lax.rem(x + k, SIDE) * PIECE, PIECE)
                copies.append(
                    copy(
                        acc.at[ch, pl.ds(at, PIECE)], parts.at[ch, s, k - 1],
                        rss.at[0], rsr.at[ch, s], pix_to(k),
                    )
                )
        return copies

    def gather_start(ch, s, copies):
        with jax.named_scope(f"gather{ch}{s}"):
            here = pl.multiple_of(mine + s * SUB + x * PIECE, PIECE)
            remote(parts.at[ch, s], parts.at[ch, s], rss.at[0], rsr.at[ch, s], partner).wait_recv()
            total = acc[ch, pl.ds(here, PIECE), :]
            for k in range(1, SIDE):
                total += parts[ch, s, k - 1]
            out[ch, pl.ds(here, PIECE), :] = total
            block = out.at[ch, pl.ds(here, PIECE)]
            gathers = [
                (k, copy(block, block, ags.at[0], agr.at[ch, s, k - 1], pix_to(k))) for k in (2, 1, 3)
            ]
        return gathers, [copy(block, block, fws.at[0], fwr.at[ch], partner)]

    def forward(ch, s, started_gathers):
        gathers, sent = started_gathers
        with jax.named_scope(f"forward{ch}{s}"):
            for k, c in (gathers[1], gathers[2], gathers[0]):
                c.wait_recv()
                at = pl.multiple_of(mine + s * SUB + lax.rem(x - k + SIDE, SIDE) * PIECE, PIECE)
                block = out.at[ch, pl.ds(at, PIECE)]
                copy(block, block, fws.at[0], fwr.at[ch], partner)
        return sent

    for g in range(3):
        combine(0, g)
    s0 = combine_swap(0, 3)
    r0 = [reduce_start(0, s, s0[s]) for s in range(SUBS)]
    combine(1, 0)
    combine(1, 1)
    combine(1, 2)
    g0 = [gather_start(0, s, r0[s]) for s in range(SUBS)]
    s1 = combine_swap(1, 3)
    r1 = [reduce_start(1, s, s1[s]) for s in range(SUBS)]
    f0 = [forward(0, s, g0[s]) for s in range(SUBS)]
    g1 = [gather_start(1, s, r1[s]) for s in range(SUBS)]
    f1 = [forward(1, s, g1[s]) for s in range(SUBS)]
    with jax.named_scope("last"):
        for ch in range(2):
            block = out.at[ch, pl.ds(pl.multiple_of(theirs, HALF), HALF)]
            remote(block, block, fws.at[0], fwr.at[ch], partner).wait_recv()
        for whole, sem in (
            (send.at[pl.ds(1, N_VOL - 1), pl.ds(0, CAP + 1)], p1s),
            (send.at[pl.ds(1, N_VOL - 1), pl.ds(FIRST, CAP)], p1s),
            (other, d2s),
            (parts, rss),
            (parts, ags),
            (out.at[:, pl.ds(0, HALF)], fws),
        ):
            remote(whole, whole, sem.at[0], d2r.at[0, 0], partner).wait_send()


def exchange(partial, pick, ids):
    vmem = pl.BlockSpec(memory_space=pltpu.VMEM)
    dma = pltpu.SemaphoreType.DMA
    return pl.pallas_call(
        exchange_kernel,
        out_shape=jax.ShapeDtypeStruct((2, BLOCK_TILES, LANES), F32),
        in_specs=[vmem] * 3,
        out_specs=vmem,
        scratch_shapes=[
            pltpu.VMEM((N_VOL, MSG, LANES), F32),
            pltpu.VMEM((N_VOL, MSG, LANES), F32),
            pltpu.VMEM((2, BLOCK_TILES, LANES), F32),
            pltpu.VMEM((2, SUBS, SUB, LANES), F32),
            pltpu.VMEM((2, SUBS, SIDE - 1, PIECE, LANES), F32),
            pltpu.VMEM((GROUP * CAP, 2 * LANES), BF16),
            pltpu.VMEM((BLOCK_TILES, N_VOL * CAP), BF16),
            dma((1,)), dma((2, N_VOL // GROUP)),
            dma((1,)), dma((2, SUBS)),
            dma((1,)), dma((2, SUBS)),
            dma((1,)), dma((2, SUBS, SIDE - 1)),
            dma((1,)), dma((2,)),
        ],
        compiler_params=pltpu.CompilerParams(
            collective_id=0, has_side_effects=True, vmem_limit_bytes=32 << 20
        ),
        name="exchange",
    )(partial, pick, ids)


def finish_kernel(map_ref, owner_ref, owned_h, shell_h, owned, rhs, sems):
    vol = lax.axis_index("vol")
    pix = lax.axis_index("pix")
    copies = []
    for ch in range(2):
        c = pltpu.make_async_copy(
            map_ref.at[ch], shell_h.at[:, pl.ds(ch * LANES, LANES)], sems.at[ch]
        )
        c.start()
        copies.append(c)
    rows = BLOCK_TILES // LANES
    owner = owner_ref[pl.ds(pl.multiple_of(vol * rows, rows), rows), :]
    match = (owner == pix).astype(F32).astype(BF16)
    before = (iota((LANES, LANES), 0) < iota((LANES, LANES), 1)).astype(F32).astype(BF16)
    above = (iota((rows, rows), 1) < iota((rows, rows), 0)).astype(F32).astype(BF16)
    ones = jnp.ones((LANES, LANES), BF16)
    rank = dot(match, before) + dot(dot(above, match).astype(BF16), ones)
    key = jnp.where(match.astype(F32) > 0, rank, -1.0)
    for ch in range(2):
        high, low = halves(map_ref[ch])
        rhs[:, ch * LANES : (ch + 1) * LANES] = high
        rhs[:, (ch + 2) * LANES : (ch + 3) * LANES] = low
    place = iota((BAND, LANES), 0).astype(F32).astype(BF16)
    for t in range(OWN_MAX // BAND):
        local = key - t * BAND
        local = jnp.where((local >= 0) & (local < BAND), local, -1.0).astype(BF16)
        chosen = jnp.concatenate([equal(place, local[g : g + 1]) for g in range(rows)], 1)
        both = dot(chosen, rhs[...])
        here = pl.ds(t * BAND, BAND)
        owned[here, :] = both[:, : 2 * LANES] + both[:, 2 * LANES :]
        c = pltpu.make_async_copy(owned.at[here], owned_h.at[here], sems.at[2 + t])
        c.start()
        copies.append(c)
    for c in copies:
        c.wait()


def finish(block_map, tile_owner):
    vmem = pl.BlockSpec(memory_space=pltpu.VMEM)
    return pl.pallas_call(
        finish_kernel,
        out_shape=(
            jax.ShapeDtypeStruct((OWN_MAX, 2 * LANES), F32),
            jax.ShapeDtypeStruct((BLOCK_TILES, 2 * LANES), F32),
        ),
        in_specs=[vmem, vmem],
        out_specs=(pl.BlockSpec(memory_space=pltpu.HBM),) * 2,
        scratch_shapes=[
            pltpu.VMEM((OWN_MAX, 2 * LANES), F32),
            pltpu.VMEM((BLOCK_TILES, 4 * LANES), BF16),
            pltpu.SemaphoreType.DMA((2 + OWN_MAX // BAND,)),
        ],
        compiler_params=pltpu.CompilerParams(vmem_limit_bytes=16 << 20),
        name="finish",
    )(block_map, tile_owner)


def shards(kernel, pressure, velocity, entry_slot, slot_tile, tile_owner):
    square = (ENTRIES // LANES, LANES)
    partial, pick, ids = project(
        kernel,
        pressure.reshape(square),
        velocity.reshape(square),
        entry_slot.reshape(square),
        slot_tile.reshape(SLOTS // LANES, LANES),
    )
    block_map = exchange(partial, pick, ids)
    return finish(block_map, tile_owner.reshape(-1, LANES))


def solution(mesh):
    in_specs = (
        P(("vol", "pix"), None),
        P(("vol", "pix")),
        P(("vol", "pix")),
        P(("vol", "pix"), None),
        P(("vol", "pix"), None),
        P(),
    )
    out_specs = (P(("vol", "pix"), None), P("vol", None))
    return jax.shard_map(shards, mesh=mesh, in_specs=in_specs, out_specs=out_specs, check_vma=False)
```

```python
import functools

import jax
import jax.numpy as jnp
from jax import lax
from jax.experimental import pallas as pl
from jax.experimental.pallas import tpu as pltpu
from jax.sharding import PartitionSpec as P

MESH = pl.DeviceIdType.MESH
F32 = jnp.float32
BF16 = jnp.bfloat16

LANES = 128
ENTRIES = 16384
SLOTS = 1024
N_VOL = 16
SIDE = 4
BLOCK_TILES = 2048
CAP = 128
OWN_MAX = 512

STEP = 8192
SPAN = 256
WINDOW = 32
MSG = 2 * CAP + 8
FIRST = CAP + 8


def dot(a, b):
    return jnp.dot(a, b, preferred_element_type=F32)


def iota(shape, dim):
    return lax.broadcasted_iota(jnp.int32, shape, dim)


def halves(x):
    high = x.astype(BF16)
    return high, (x - high.astype(F32)).astype(BF16)


def equal(place, row):
    return jnp.where(place == row, jnp.ones((), BF16), jnp.zeros((), BF16))


def project_kernel(
    kernel_h, pressure_h, velocity_h, slot_h, tile_h, rhs_ref, pick_ref, ids_ref,
    weights, pressure, velocity, slot_v, tile_v, slot_s, acc, sems, chunk_sems,
):
    steps = ENTRIES // STEP
    rows = STEP // LANES
    small = [
        pltpu.make_async_copy(a, b, sems.at[n])
        for n, (a, b) in enumerate(
            (
                (tile_h, tile_v), (slot_h, slot_s), (slot_h, slot_v),
                (pressure_h, pressure), (velocity_h, velocity),
            )
        )
    ]
    for c in small:
        c.start()

    def chunk(g):
        span = pl.ds(pl.multiple_of(g * STEP, STEP), STEP)
        return pltpu.make_async_copy(kernel_h.at[span], weights.at[span], chunk_sems.at[g])

    for g in range(steps):
        chunk(g).start()
    acc[...] = jnp.zeros_like(acc)

    small[0].wait()
    tiles = tile_v[...]
    block = tiles // BLOCK_TILES
    within = tiles - block * BLOCK_TILES
    groups = SLOTS // LANES
    match = jnp.concatenate([(block == v).astype(F32) for v in range(N_VOL)], 0)
    r, c = iota((LANES, LANES), 0), iota((LANES, LANES), 1)
    before = (r < c).astype(F32).astype(BF16)
    above = ((c < r) & (c // groups == r // groups)).astype(F32).astype(BF16)
    ones = jnp.ones((LANES, LANES), BF16)
    packed = match.astype(BF16)
    rank = dot(packed, before) + dot(dot(above, packed).astype(BF16), ones)
    key = jnp.where(match > 0, rank, -1.0).astype(BF16)
    own = jnp.zeros((groups, LANES), F32)
    for v in range(N_VOL):
        own += match[v * groups : (v + 1) * groups] * rank[v * groups : (v + 1) * groups]
    place = iota((LANES, LANES), 0).astype(F32).astype(BF16)
    spread = jnp.concatenate([equal(place, own[g : g + 1].astype(BF16)) for g in range(groups)], 1)
    for v in range(N_VOL):
        for g in range(groups):
            row = v * groups + g
            pick_ref[v * CAP : (v + 1) * CAP, g * LANES : (g + 1) * LANES] = equal(place, key[row : row + 1])
    vols = iota((N_VOL, LANES), 0)
    upper, lower = (within // 64).astype(F32), (within % 64).astype(F32)
    table = []
    for values in (upper, lower, jnp.ones_like(upper)):
        table.append(
            jnp.concatenate(
                [jnp.where(vols == block[g : g + 1], values[g : g + 1], 0.0) for g in range(groups)], 1
            )
        )
    table = jnp.concatenate(table, 0).astype(BF16)
    found = lax.dot_general(table, spread, (((1,), (1,)), ((), ())), preferred_element_type=F32)
    ids_ref[...] = found[:N_VOL] * 64.0 + found[N_VOL : 2 * N_VOL] + found[2 * N_VOL :] - 1.0

    for n in (1, 2, 3, 4):
        small[n].wait()
    lines = iota((WINDOW, LANES), 0)
    per = SPAN // LANES

    @pl.loop(0, steps)
    def _(g):
        chunk(g).wait()
        top = pl.multiple_of(g * rows, rows)
        thermal = pressure[pl.ds(top, rows), :].astype(F32)
        kinetic = velocity[pl.ds(top, rows), :].astype(F32)
        slots = slot_v[pl.ds(top, rows), :]

        def products(i, base):
            up, low = [], []
            for h in range(per):
                n = i * per + h
                match = lines == slots[n : n + 1, :] - base
                up.append(jnp.where(match, thermal[n : n + 1, :], 0.0))
                low.append(jnp.where(match, kinetic[n : n + 1, :], 0.0))
            amplitudes = jnp.concatenate([jnp.concatenate(up, 1), jnp.concatenate(low, 1)], 0)
            span = pl.ds(pl.multiple_of(g * STEP + i * SPAN, SPAN), SPAN)
            return dot(amplitudes.astype(BF16), weights[span, :])

        def add(base, value):
            acc[0, pl.ds(base, WINDOW), :] += value[:WINDOW]
            acc[1, pl.ds(base, WINDOW), :] += value[WINDOW:]

        count = STEP // SPAN
        bases, lasts = [], []
        for i in range(count):
            bases.append(pl.multiple_of(slot_s[top + i * per, 0] & -8, 8))
            lasts.append(slot_s[top + i * per + per - 1, LANES - 1])
        values = [products(i, bases[i]) for i in range(count)]
        for i in range(count):
            add(bases[i], values[i])
        widest = lasts[0] - bases[0]
        for i in range(1, count):
            widest = jnp.maximum(widest, lasts[i] - bases[i])

        @pl.when(widest >= WINDOW)
        def _():
            for i in range(count):

                @pl.loop(1, (lasts[i] - bases[i]) // WINDOW + 1)
                def _(w, i=i):
                    base = pl.multiple_of(bases[i] + w * WINDOW, 8)
                    add(base, products(i, base))

    for ch in range(2):
        high, low = halves(acc[ch, :SLOTS, :])
        rhs_ref[:, 2 * ch * LANES : (2 * ch + 1) * LANES] = high
        rhs_ref[:, (2 * ch + 1) * LANES : (2 * ch + 2) * LANES] = low


def project(kernel, pressure, velocity, entry_slot, slot_tile):
    outs = (((SLOTS, 4 * LANES), BF16), ((N_VOL * CAP, SLOTS), BF16), ((N_VOL, LANES), F32))
    square = (ENTRIES // LANES, LANES)
    return pl.pallas_call(
        project_kernel,
        out_shape=tuple(jax.ShapeDtypeStruct(*o) for o in outs),
        in_specs=[pl.BlockSpec(memory_space=pltpu.HBM)] * 5,
        out_specs=tuple(pl.BlockSpec(memory_space=pltpu.VMEM) for o in outs),
        scratch_shapes=[
            pltpu.VMEM((ENTRIES, LANES), BF16),
            pltpu.VMEM(square, BF16),
            pltpu.VMEM(square, BF16),
            pltpu.VMEM(square, jnp.int32),
            pltpu.VMEM((SLOTS // LANES, LANES), jnp.int32),
            pltpu.SMEM(square, jnp.int32),
            pltpu.VMEM((2, SLOTS + WINDOW + 8, LANES), F32),
            pltpu.SemaphoreType.DMA((5,)),
            pltpu.SemaphoreType.DMA((ENTRIES // STEP,)),
        ],
        compiler_params=pltpu.CompilerParams(vmem_limit_bytes=16 << 20),
        name="project",
    )(*(pltpu.with_memory_space_constraint(a, pltpu.HBM) for a in (kernel, pressure, velocity, entry_slot, slot_tile)))


GROUP = 4
SUBS = 2
HALF = BLOCK_TILES // 2
SUB = HALF // SUBS
PIECE = SUB // SIDE
TALL = 1024
BAND = 256
ORDER = (0, 4, 12, 1, 3, 8, 2, 5, 7, 13, 15, 9, 11, 6, 14, 10)
ROUND = 16


def exchange_kernel(
    partial, pick, ids_ref, owner_ref, out, own0, own_hot, send, recv, acc, other, parts, rhs, hot, split,
    p1s, p1r, d2s, d2r, rss, rsr, ags, agr, fws, fwr,
):
    vol = lax.axis_index("vol")
    pix = lax.axis_index("pix")
    x, core = pix // 2, pix % 2
    y, z = vol // SIDE, vol % SIDE

    def vol_to(k):
        return lax.rem(y + k // SIDE, SIDE) * SIDE + lax.rem(z + k % SIDE, SIDE)

    def pix_to(k):
        return {"pix": lax.rem(x + k, SIDE) * 2 + core}

    partner = {"pix": x * 2 + 1 - core}
    peers = [{"vol": vol_to(k)} for k in range(1, N_VOL)] + [pix_to(k) for k in range(1, SIDE)] + [partner]
    barrier = pltpu.get_barrier_semaphore()
    for peer in peers:
        pl.semaphore_signal(barrier, inc=1, device_id=peer, device_id_type=MESH)

    def remote(src, dst, s, r, peer):
        return pltpu.make_async_remote_copy(
            src_ref=src, dst_ref=dst, send_sem=s, recv_sem=r, device_id=peer, device_id_type=MESH
        )

    def copy(src, dst, s, r, peer):
        c = remote(src, dst, s, r, peer)
        c.start()
        return c

    spans = ((0, CAP + 1), (FIRST, CAP))
    rows_of = (0, FIRST)
    def launch(ch, n):
        begin, size = spans[ch]
        copy(
            send.at[n, pl.ds(begin, size)],
            recv.at[n, pl.ds(begin, size)],
            p1s.at[0], p1r.at[ch, n // GROUP], {"vol": vol_to(ORDER[n])},
        )

    def arrived(ch, group):
        begin, size = spans[ch]
        low = max(group * GROUP, 1)
        span = pl.ds(low, (group + 1) * GROUP - low)
        span = recv.at[span, pl.ds(begin, size)]
        remote(span, span, p1s.at[0], p1r.at[ch, group], partner).wait_recv()

    def batch(ch, ns):
        rows = []
        for n in ns:
            to = vol_to(ORDER[n])
            rows.append(pick[pl.ds(pl.multiple_of(to * CAP, CAP), CAP), :])
            if ch == 0:
                send[n, CAP:FIRST, :] = jnp.broadcast_to(ids_ref[pl.ds(to, 1), :], (8, LANES))
        both = dot(jnp.concatenate(rows, 0), partial[:, 2 * ch * LANES : 2 * (ch + 1) * LANES])
        total = both[:, :LANES] + both[:, LANES:]
        for m, n in enumerate(ns):
            send[n, rows_of[ch] : rows_of[ch] + CAP, :] = total[m * CAP : (m + 1) * CAP]

    todo = tuple(range(1, N_VOL)) + (0,)
    with jax.named_scope("messages"):
        for n in range(0, N_VOL, ROUND):
            batch(0, todo[n : n + ROUND])
        pl.semaphore_wait(barrier, len(peers))
        for n in range(1, N_VOL):
            launch(0, n)
        for n in range(0, N_VOL, ROUND):
            batch(1, todo[n : n + ROUND])

    def launch_second():
        for n in range(1, N_VOL):
            launch(1, n)

    band = iota((BAND, LANES), 0).astype(F32).astype(BF16)
    mine = core * HALF
    theirs = HALF - mine
    turn = GROUP * CAP

    def load(ch, group):
        ids = []
        arrived(ch, group)
        if ch == 0 and group == 1:
            launch_second()
        for n in range(GROUP):
            k = group * GROUP + n
            source = recv if k else send
            ids.append(source[k, CAP : CAP + 1, :])
            high, low = halves(source[k, rows_of[ch] : rows_of[ch] + CAP, :])
            rhs[n * CAP : (n + 1) * CAP, :LANES] = high
            rhs[n * CAP : (n + 1) * CAP, LANES:] = low
        return ids

    def tiles(ch, group, ids, begin, count):
        columns = slice(group * turn, (group + 1) * turn)

        def one(t):
            at = pl.multiple_of(begin + t * TALL, TALL)
            if ch == 0:
                for b in range(TALL // BAND):
                    low = pl.multiple_of(at + b * BAND, BAND)
                    pieces = []
                    for i in ids:
                        local = i - low.astype(F32)
                        local = jnp.where((local >= 0) & (local < BAND), local, -1.0)
                        pieces.append(equal(band, local.astype(BF16)))
                    hot[pl.ds(low, BAND), columns] = jnp.concatenate(pieces, 1)
            both = dot(hot[pl.ds(at, TALL), columns], rhs[...])
            total = both[:, :LANES] + both[:, LANES:]
            if group:
                total += acc[ch, pl.ds(at, TALL), :]
            acc[ch, pl.ds(at, TALL), :] = total

        if count == 1:
            one(0)
        else:
            pl.loop(0, count)(one)

    def combine(ch, group):
        with jax.named_scope(f"load{ch}{group}"):
            ids = load(ch, group)
        with jax.named_scope(f"combine{ch}{group}"):
            tiles(ch, group, ids, jnp.int32(0), BLOCK_TILES // TALL)

    def combine_swap(ch, group):
        with jax.named_scope(f"load{ch}{group}"):
            ids = load(ch, group)
        copies = []
        with jax.named_scope(f"combine{ch}{group}"):
            tiles(ch, group, ids, theirs, HALF // TALL)
            for s in range(SUBS):
                at = pl.multiple_of(theirs + s * SUB, SUB)
                copies.append(
                    copy(acc.at[ch, pl.ds(at, SUB)], other.at[ch, s], d2s.at[0], d2r.at[ch, s], partner)
                )
            tiles(ch, group, ids, mine, HALF // TALL)
        return copies

    def reduce_start(ch, s, swapped):
        with jax.named_scope(f"reduce{ch}{s}"):
            swapped.wait_recv()
            acc[ch, pl.ds(pl.multiple_of(mine + s * SUB, SUB), SUB), :] += other[ch, s]
            copies = []
            for k in (2, 1, 3):
                at = pl.multiple_of(mine + s * SUB + lax.rem(x + k, SIDE) * PIECE, PIECE)
                copies.append(
                    copy(
                        acc.at[ch, pl.ds(at, PIECE)], parts.at[ch, s, k - 1],
                        rss.at[0], rsr.at[ch, s], pix_to(k),
                    )
                )
        return copies

    def gather_start(ch, s, copies):
        with jax.named_scope(f"gather{ch}{s}"):
            here = pl.multiple_of(mine + s * SUB + x * PIECE, PIECE)
            remote(parts.at[ch, s], parts.at[ch, s], rss.at[0], rsr.at[ch, s], partner).wait_recv()
            total = acc[ch, pl.ds(here, PIECE), :]
            for k in range(1, SIDE):
                total += parts[ch, s, k - 1]
            out[ch, pl.ds(here, PIECE), :] = total
            block = out.at[ch, pl.ds(here, PIECE)]
            gathers = [
                (k, copy(block, block, ags.at[0], agr.at[ch, s, k - 1], pix_to(k))) for k in (2, 1, 3)
            ]
        return gathers, [copy(block, block, fws.at[0], fwr.at[ch], partner)]

    def forward(ch, s, started_gathers):
        gathers, sent = started_gathers
        with jax.named_scope(f"forward{ch}{s}"):
            for k, c in (gathers[1], gathers[2], gathers[0]):
                c.wait_recv()
                at = pl.multiple_of(mine + s * SUB + lax.rem(x - k + SIDE, SIDE) * PIECE, PIECE)
                block = out.at[ch, pl.ds(at, PIECE)]
                copy(block, block, fws.at[0], fwr.at[ch], partner)
        return sent

    def settled(ch):
        block = out.at[ch, pl.ds(pl.multiple_of(theirs, HALF), HALF)]
        remote(block, block, fws.at[0], fwr.at[ch], partner).wait_recv()

    def owned_places():
        with jax.named_scope("places"):
            rows = BLOCK_TILES // LANES
            owner = owner_ref[pl.ds(pl.multiple_of(vol * rows, rows), rows), :]
            match = (owner == pix).astype(F32)
            packed = match.astype(BF16)
            before = (iota((LANES, LANES), 0) < iota((LANES, LANES), 1)).astype(F32).astype(BF16)
            above = (iota((rows, rows), 1) < iota((rows, rows), 0)).astype(F32).astype(BF16)
            ones = jnp.ones((LANES, LANES), BF16)
            rank = dot(packed, before) + dot(dot(above, packed).astype(BF16), ones)
            key = jnp.where(match > 0, rank, -1.0)
            for t in range(OWN_MAX // BAND):
                local = key - t * BAND
                local = jnp.where((local >= 0) & (local < BAND), local, -1.0).astype(BF16)
                for g in range(rows):
                    own_hot[t * BAND : (t + 1) * BAND, g * LANES : (g + 1) * LANES] = equal(band, local[g : g + 1])

    def owned_first():
        with jax.named_scope("owned"):
            settled(0)
            high, low = halves(out[0])
            split[:, :LANES] = high
            split[:, LANES:] = low
            both = dot(own_hot[...], split[...])
            own0[...] = both[:, :LANES] + both[:, LANES:]

    subs = range(SUBS)
    combine(0, 0)
    owned_places()
    combine(0, 1)
    combine(0, 2)
    s0 = combine_swap(0, 3)
    r0 = [reduce_start(0, s, s0[s]) for s in subs]
    combine(1, 0)
    combine(1, 1)
    g0 = [gather_start(0, 0, r0[0])]
    combine(1, 2)
    g0.append(gather_start(0, 1, r0[1]))
    s1 = combine_swap(1, 3)
    r1 = [reduce_start(1, s, s1[s]) for s in subs]
    f0 = [forward(0, s, g0[s]) for s in subs]
    g1 = [gather_start(1, 0, r1[0])]
    owned_first()
    g1.append(gather_start(1, 1, r1[1]))
    f1 = [forward(1, s, g1[s]) for s in subs]
    with jax.named_scope("last"):
        settled(1)
        for whole, sem in (
            (send.at[pl.ds(1, N_VOL - 1), pl.ds(0, CAP + 1)], p1s),
            (send.at[pl.ds(1, N_VOL - 1), pl.ds(FIRST, CAP)], p1s),
            (other, d2s),
            (parts, rss),
            (parts, ags),
            (out.at[:, pl.ds(0, HALF)], fws),
        ):
            remote(whole, whole, sem.at[0], d2r.at[0, 0], partner).wait_send()


def exchange(partial, pick, ids, tile_owner):
    vmem = pl.BlockSpec(memory_space=pltpu.VMEM)
    dma = pltpu.SemaphoreType.DMA
    return pl.pallas_call(
        exchange_kernel,
        out_shape=(
            jax.ShapeDtypeStruct((2, BLOCK_TILES, LANES), F32),
            jax.ShapeDtypeStruct((OWN_MAX, LANES), F32),
            jax.ShapeDtypeStruct((OWN_MAX, BLOCK_TILES), BF16),
        ),
        in_specs=[vmem] * 4,
        out_specs=(vmem,) * 3,
        scratch_shapes=[
            pltpu.VMEM((N_VOL, MSG, LANES), F32),
            pltpu.VMEM((N_VOL, MSG, LANES), F32),
            pltpu.VMEM((2, BLOCK_TILES, LANES), F32),
            pltpu.VMEM((2, SUBS, SUB, LANES), F32),
            pltpu.VMEM((2, SUBS, SIDE - 1, PIECE, LANES), F32),
            pltpu.VMEM((GROUP * CAP, 2 * LANES), BF16),
            pltpu.VMEM((BLOCK_TILES, N_VOL * CAP), BF16),
            pltpu.VMEM((BLOCK_TILES, 2 * LANES), BF16),
            dma((1,)), dma((2, N_VOL // GROUP)),
            dma((1,)), dma((2, SUBS)),
            dma((1,)), dma((2, SUBS)),
            dma((1,)), dma((2, SUBS, SIDE - 1)),
            dma((1,)), dma((2,)),
        ],
        compiler_params=pltpu.CompilerParams(
            collective_id=0, has_side_effects=True, vmem_limit_bytes=32 << 20
        ),
        name="exchange",
    )(partial, pick, ids, tile_owner)


def finish_kernel(map_ref, own0, own_hot, owned_h, shell_h, owned, rhs, sems):
    def put(source, target, n):
        c = pltpu.make_async_copy(source, target, sems.at[n])
        c.start()
        return c

    left, right = pl.ds(0, LANES), pl.ds(LANES, LANES)
    copies = [
        put(map_ref.at[1], shell_h.at[:, right], 0),
        put(map_ref.at[0], shell_h.at[:, left], 1),
        put(own0, owned_h.at[:, left], 2),
    ]
    high, low = halves(map_ref[1])
    rhs[:, :LANES] = high
    rhs[:, LANES:] = low
    both = dot(own_hot[...], rhs[...])
    owned[...] = both[:, :LANES] + both[:, LANES:]
    copies.append(put(owned, owned_h.at[:, right], 3))
    for c in copies:
        c.wait()


def finish(block_map, own0, own_hot):
    vmem = pl.BlockSpec(memory_space=pltpu.VMEM)
    return pl.pallas_call(
        finish_kernel,
        out_shape=(
            jax.ShapeDtypeStruct((OWN_MAX, 2 * LANES), F32),
            jax.ShapeDtypeStruct((BLOCK_TILES, 2 * LANES), F32),
        ),
        in_specs=[vmem] * 3,
        out_specs=(pl.BlockSpec(memory_space=pltpu.HBM),) * 2,
        scratch_shapes=[
            pltpu.VMEM((OWN_MAX, LANES), F32),
            pltpu.VMEM((BLOCK_TILES, 2 * LANES), BF16),
            pltpu.SemaphoreType.DMA((4,)),
        ],
        compiler_params=pltpu.CompilerParams(vmem_limit_bytes=16 << 20),
        name="finish",
    )(block_map, own0, own_hot)


def shards(kernel, pressure, velocity, entry_slot, slot_tile, tile_owner):
    square = (ENTRIES // LANES, LANES)
    partial, pick, ids = project(
        kernel,
        pressure.reshape(square),
        velocity.reshape(square),
        entry_slot.reshape(square),
        slot_tile.reshape(SLOTS // LANES, LANES),
    )
    block_map, own0, own_hot = exchange(partial, pick, ids, tile_owner.reshape(-1, LANES))
    return finish(block_map, own0, own_hot)


def solution(mesh):
    in_specs = (
        P(("vol", "pix"), None),
        P(("vol", "pix")),
        P(("vol", "pix")),
        P(("vol", "pix"), None),
        P(("vol", "pix"), None),
        P(),
    )
    out_specs = (P(("vol", "pix"), None), P("vol", None))
    return jax.shard_map(shards, mesh=mesh, in_specs=in_specs, out_specs=out_specs, check_vma=False)
```

```python
import functools

import jax
import jax.numpy as jnp
from jax import lax
from jax.experimental import pallas as pl
from jax.experimental.pallas import tpu as pltpu
from jax.sharding import PartitionSpec as P

MESH = pl.DeviceIdType.MESH
F32 = jnp.float32
BF16 = jnp.bfloat16

LANES = 128
ENTRIES = 16384
SLOTS = 1024
N_VOL = 16
SIDE = 4
BLOCK_TILES = 2048
CAP = 128
OWN_MAX = 512

STEP = 8192
SPAN = 256
WINDOW = 40
MSG = 2 * CAP + 8
FIRST = CAP + 8


def dot(a, b):
    return jnp.dot(a, b, preferred_element_type=F32)


def iota(shape, dim):
    return lax.broadcasted_iota(jnp.int32, shape, dim)


def halves(x):
    high = x.astype(BF16)
    return high, (x - high.astype(F32)).astype(BF16)


def equal(place, row):
    return jnp.where(place == row, jnp.ones((), BF16), jnp.zeros((), BF16))


def project_kernel(
    kernel_h, pressure_h, velocity_h, slot_h, tile_h, rhs_ref, pick_ref, ids_ref,
    weights, pressure, velocity, slot_v, tile_v, slot_s, acc, sems, chunk_sems,
):
    steps = ENTRIES // STEP
    rows = STEP // LANES
    small = [
        pltpu.make_async_copy(a, b, sems.at[n])
        for n, (a, b) in enumerate(
            (
                (tile_h, tile_v), (slot_h, slot_s), (slot_h, slot_v),
                (pressure_h, pressure), (velocity_h, velocity),
            )
        )
    ]
    for c in small:
        c.start()

    def chunk(g):
        span = pl.ds(pl.multiple_of(g * STEP, STEP), STEP)
        return pltpu.make_async_copy(kernel_h.at[span], weights.at[span], chunk_sems.at[g])

    for g in range(steps):
        chunk(g).start()
    acc[...] = jnp.zeros_like(acc)

    small[0].wait()
    tiles = tile_v[...]
    block = tiles // BLOCK_TILES
    within = tiles - block * BLOCK_TILES
    groups = SLOTS // LANES
    match = jnp.concatenate([(block == v).astype(F32) for v in range(N_VOL)], 0)
    r, c = iota((LANES, LANES), 0), iota((LANES, LANES), 1)
    before = (r < c).astype(F32).astype(BF16)
    above = ((c < r) & (c // groups == r // groups)).astype(F32).astype(BF16)
    ones = jnp.ones((LANES, LANES), BF16)
    packed = match.astype(BF16)
    rank = dot(packed, before) + dot(dot(above, packed).astype(BF16), ones)
    key = jnp.where(match > 0, rank, -1.0).astype(BF16)
    own = jnp.zeros((groups, LANES), F32)
    for v in range(N_VOL):
        own += match[v * groups : (v + 1) * groups] * rank[v * groups : (v + 1) * groups]
    place = iota((LANES, LANES), 0).astype(F32).astype(BF16)
    spread = jnp.concatenate([equal(place, own[g : g + 1].astype(BF16)) for g in range(groups)], 1)
    for v in range(N_VOL):
        for g in range(groups):
            row = v * groups + g
            pick_ref[v * CAP : (v + 1) * CAP, g * LANES : (g + 1) * LANES] = equal(place, key[row : row + 1])
    vols = iota((N_VOL, LANES), 0)
    upper, lower = (within // 64).astype(F32), (within % 64).astype(F32)
    table = []
    for values in (upper, lower, jnp.ones_like(upper)):
        table.append(
            jnp.concatenate(
                [jnp.where(vols == block[g : g + 1], values[g : g + 1], 0.0) for g in range(groups)], 1
            )
        )
    table = jnp.concatenate(table, 0).astype(BF16)
    found = lax.dot_general(table, spread, (((1,), (1,)), ((), ())), preferred_element_type=F32)
    ids_ref[...] = found[:N_VOL] * 64.0 + found[N_VOL : 2 * N_VOL] + found[2 * N_VOL :] - 1.0

    for n in (1, 2, 3, 4):
        small[n].wait()
    lines = iota((WINDOW, LANES), 0)
    per = SPAN // LANES

    @pl.loop(0, steps)
    def _(g):
        chunk(g).wait()
        top = pl.multiple_of(g * rows, rows)
        thermal = pressure[pl.ds(top, rows), :].astype(F32)
        kinetic = velocity[pl.ds(top, rows), :].astype(F32)
        slots = slot_v[pl.ds(top, rows), :]

        def products(i, base):
            up, low = [], []
            for h in range(per):
                n = i * per + h
                match = lines == slots[n : n + 1, :] - base
                up.append(jnp.where(match, thermal[n : n + 1, :], 0.0))
                low.append(jnp.where(match, kinetic[n : n + 1, :], 0.0))
            amplitudes = jnp.concatenate([jnp.concatenate(up, 1), jnp.concatenate(low, 1)], 0)
            span = pl.ds(pl.multiple_of(g * STEP + i * SPAN, SPAN), SPAN)
            return dot(amplitudes.astype(BF16), weights[span, :])

        def add(base, value):
            acc[0, pl.ds(base, WINDOW), :] += value[:WINDOW]
            acc[1, pl.ds(base, WINDOW), :] += value[WINDOW:]

        count = STEP // SPAN
        bases, lasts = [], []
        for i in range(count):
            bases.append(pl.multiple_of(slot_s[top + i * per, 0] & -8, 8))
            lasts.append(slot_s[top + i * per + per - 1, LANES - 1])
        values = [products(i, bases[i]) for i in range(count)]
        for i in range(count):
            add(bases[i], values[i])
        widest = lasts[0] - bases[0]
        for i in range(1, count):
            widest = jnp.maximum(widest, lasts[i] - bases[i])

        @pl.when(widest >= WINDOW)
        def _():
            for i in range(count):

                @pl.loop(1, (lasts[i] - bases[i]) // WINDOW + 1)
                def _(w, i=i):
                    base = pl.multiple_of(bases[i] + w * WINDOW, 8)
                    add(base, products(i, base))

    for ch in range(2):
        high, low = halves(acc[ch, :SLOTS, :])
        rhs_ref[:, 2 * ch * LANES : (2 * ch + 1) * LANES] = high
        rhs_ref[:, (2 * ch + 1) * LANES : (2 * ch + 2) * LANES] = low


def project(kernel, pressure, velocity, entry_slot, slot_tile):
    outs = (((SLOTS, 4 * LANES), BF16), ((N_VOL * CAP, SLOTS), BF16), ((N_VOL, LANES), F32))
    square = (ENTRIES // LANES, LANES)
    return pl.pallas_call(
        project_kernel,
        out_shape=tuple(jax.ShapeDtypeStruct(*o) for o in outs),
        in_specs=[pl.BlockSpec(memory_space=pltpu.HBM)] * 5,
        out_specs=tuple(pl.BlockSpec(memory_space=pltpu.VMEM) for o in outs),
        scratch_shapes=[
            pltpu.VMEM((ENTRIES, LANES), BF16),
            pltpu.VMEM(square, BF16),
            pltpu.VMEM(square, BF16),
            pltpu.VMEM(square, jnp.int32),
            pltpu.VMEM((SLOTS // LANES, LANES), jnp.int32),
            pltpu.SMEM(square, jnp.int32),
            pltpu.VMEM((2, SLOTS + WINDOW + 8, LANES), F32),
            pltpu.SemaphoreType.DMA((5,)),
            pltpu.SemaphoreType.DMA((ENTRIES // STEP,)),
        ],
        compiler_params=pltpu.CompilerParams(vmem_limit_bytes=16 << 20),
        name="project",
    )(*(pltpu.with_memory_space_constraint(a, pltpu.HBM) for a in (kernel, pressure, velocity, entry_slot, slot_tile)))


GROUP = 4
SUBS = 2
HALF = BLOCK_TILES // 2
SUB = HALF // SUBS
PIECE = SUB // SIDE
TALL = 1024
BAND = 256
ORDER = (0, 4, 1, 12, 3, 8, 2, 5, 15, 13, 7, 9, 6, 11, 14, 10)
ROUND = 16


def exchange_kernel(
    partial, pick, ids_ref, owner_ref, out, own0, own_hot, send, recv, acc, other, parts, rhs, hot, split,
    p1s, p1r, d2s, d2r, rss, rsr, ags, agr, fws, fwr,
):
    vol = lax.axis_index("vol")
    pix = lax.axis_index("pix")
    x, core = pix // 2, pix % 2
    y, z = vol // SIDE, vol % SIDE

    def vol_to(k):
        return lax.rem(y + k // SIDE, SIDE) * SIDE + lax.rem(z + k % SIDE, SIDE)

    def pix_to(k):
        return {"pix": lax.rem(x + k, SIDE) * 2 + core}

    partner = {"pix": x * 2 + 1 - core}
    peers = [{"vol": vol_to(k)} for k in range(1, N_VOL)] + [pix_to(k) for k in range(1, SIDE)] + [partner]
    barrier = pltpu.get_barrier_semaphore()
    for peer in peers:
        pl.semaphore_signal(barrier, inc=1, device_id=peer, device_id_type=MESH)

    def remote(src, dst, s, r, peer):
        return pltpu.make_async_remote_copy(
            src_ref=src, dst_ref=dst, send_sem=s, recv_sem=r, device_id=peer, device_id_type=MESH
        )

    def copy(src, dst, s, r, peer):
        c = remote(src, dst, s, r, peer)
        c.start()
        return c

    spans = ((0, CAP + 1), (FIRST, CAP))
    rows_of = (0, FIRST)
    def launch(ch, n):
        begin, size = spans[ch]
        copy(
            send.at[n, pl.ds(begin, size)],
            recv.at[n, pl.ds(begin, size)],
            p1s.at[0], p1r.at[ch, n // GROUP], {"vol": vol_to(ORDER[n])},
        )

    def arrived(ch, group):
        begin, size = spans[ch]
        low = max(group * GROUP, 1)
        span = pl.ds(low, (group + 1) * GROUP - low)
        span = recv.at[span, pl.ds(begin, size)]
        remote(span, span, p1s.at[0], p1r.at[ch, group], partner).wait_recv()

    def batch(ch, ns):
        rows = []
        for n in ns:
            to = vol_to(ORDER[n])
            rows.append(pick[pl.ds(pl.multiple_of(to * CAP, CAP), CAP), :])
            if ch == 0:
                send[n, CAP:FIRST, :] = jnp.broadcast_to(ids_ref[pl.ds(to, 1), :], (8, LANES))
        both = dot(jnp.concatenate(rows, 0), partial[:, 2 * ch * LANES : 2 * (ch + 1) * LANES])
        total = both[:, :LANES] + both[:, LANES:]
        for m, n in enumerate(ns):
            send[n, rows_of[ch] : rows_of[ch] + CAP, :] = total[m * CAP : (m + 1) * CAP]

    todo = tuple(range(1, N_VOL)) + (0,)
    with jax.named_scope("messages"):
        for n in range(0, N_VOL, ROUND):
            batch(0, todo[n : n + ROUND])
        pl.semaphore_wait(barrier, len(peers))
        for n in range(1, N_VOL):
            launch(0, n)
        for n in range(0, N_VOL, ROUND):
            batch(1, todo[n : n + ROUND])

    def launch_second():
        for n in range(1, N_VOL):
            launch(1, n)

    band = iota((BAND, LANES), 0).astype(F32).astype(BF16)
    mine = core * HALF
    theirs = HALF - mine
    turn = GROUP * CAP

    def load(ch, group):
        ids = []
        arrived(ch, group)
        if ch == 0 and group == 1:
            launch_second()
        for n in range(GROUP):
            k = group * GROUP + n
            source = recv if k else send
            ids.append(source[k, CAP : CAP + 1, :])
            high, low = halves(source[k, rows_of[ch] : rows_of[ch] + CAP, :])
            rhs[n * CAP : (n + 1) * CAP, :LANES] = high
            rhs[n * CAP : (n + 1) * CAP, LANES:] = low
        return ids

    def tiles(ch, group, ids, begin, count):
        columns = slice(group * turn, (group + 1) * turn)

        def one(t):
            at = pl.multiple_of(begin + t * TALL, TALL)
            if ch == 0:
                for b in range(TALL // BAND):
                    low = pl.multiple_of(at + b * BAND, BAND)
                    pieces = []
                    for i in ids:
                        local = i - low.astype(F32)
                        local = jnp.where((local >= 0) & (local < BAND), local, -1.0)
                        pieces.append(equal(band, local.astype(BF16)))
                    hot[pl.ds(low, BAND), columns] = jnp.concatenate(pieces, 1)
            both = dot(hot[pl.ds(at, TALL), columns], rhs[...])
            total = both[:, :LANES] + both[:, LANES:]
            if group:
                total += acc[ch, pl.ds(at, TALL), :]
            acc[ch, pl.ds(at, TALL), :] = total

        if count == 1:
            one(0)
        else:
            pl.loop(0, count)(one)

    def combine(ch, group):
        with jax.named_scope(f"load{ch}{group}"):
            ids = load(ch, group)
        with jax.named_scope(f"combine{ch}{group}"):
            tiles(ch, group, ids, jnp.int32(0), BLOCK_TILES // TALL)

    def combine_swap(ch, group):
        with jax.named_scope(f"load{ch}{group}"):
            ids = load(ch, group)
        copies = []
        with jax.named_scope(f"combine{ch}{group}"):
            tiles(ch, group, ids, theirs, HALF // TALL)
            for s in range(SUBS):
                at = pl.multiple_of(theirs + s * SUB, SUB)
                copies.append(
                    copy(acc.at[ch, pl.ds(at, SUB)], other.at[ch, s], d2s.at[0], d2r.at[ch, s], partner)
                )
            tiles(ch, group, ids, mine, HALF // TALL)
        return copies

    def reduce_start(ch, s, swapped):
        with jax.named_scope(f"reduce{ch}{s}"):
            swapped.wait_recv()
            acc[ch, pl.ds(pl.multiple_of(mine + s * SUB, SUB), SUB), :] += other[ch, s]
            copies = []
            for k in (2, 1, 3):
                at = pl.multiple_of(mine + s * SUB + lax.rem(x + k, SIDE) * PIECE, PIECE)
                copies.append(
                    copy(
                        acc.at[ch, pl.ds(at, PIECE)], parts.at[ch, s, k - 1],
                        rss.at[0], rsr.at[ch, s], pix_to(k),
                    )
                )
        return copies

    def gather_start(ch, s, copies):
        with jax.named_scope(f"gather{ch}{s}"):
            here = pl.multiple_of(mine + s * SUB + x * PIECE, PIECE)
            remote(parts.at[ch, s], parts.at[ch, s], rss.at[0], rsr.at[ch, s], partner).wait_recv()
            total = acc[ch, pl.ds(here, PIECE), :]
            for k in range(1, SIDE):
                total += parts[ch, s, k - 1]
            out[ch, pl.ds(here, PIECE), :] = total
            block = out.at[ch, pl.ds(here, PIECE)]
            gathers = [
                (k, copy(block, block, ags.at[0], agr.at[ch, s, k - 1], pix_to(k))) for k in (2, 1, 3)
            ]
        return gathers, [copy(block, block, fws.at[0], fwr.at[ch], partner)]

    def forward(ch, s, started_gathers):
        gathers, sent = started_gathers
        with jax.named_scope(f"forward{ch}{s}"):
            for k, c in (gathers[1], gathers[2], gathers[0]):
                c.wait_recv()
                at = pl.multiple_of(mine + s * SUB + lax.rem(x - k + SIDE, SIDE) * PIECE, PIECE)
                block = out.at[ch, pl.ds(at, PIECE)]
                copy(block, block, fws.at[0], fwr.at[ch], partner)
        return sent

    def settled(ch):
        block = out.at[ch, pl.ds(pl.multiple_of(theirs, HALF), HALF)]
        remote(block, block, fws.at[0], fwr.at[ch], partner).wait_recv()

    def owned_places():
        with jax.named_scope("places"):
            rows = BLOCK_TILES // LANES
            owner = owner_ref[pl.ds(pl.multiple_of(vol * rows, rows), rows), :]
            match = (owner == pix).astype(F32)
            packed = match.astype(BF16)
            before = (iota((LANES, LANES), 0) < iota((LANES, LANES), 1)).astype(F32).astype(BF16)
            above = (iota((rows, rows), 1) < iota((rows, rows), 0)).astype(F32).astype(BF16)
            ones = jnp.ones((LANES, LANES), BF16)
            rank = dot(packed, before) + dot(dot(above, packed).astype(BF16), ones)
            key = jnp.where(match > 0, rank, -1.0)
            for t in range(OWN_MAX // BAND):
                local = key - t * BAND
                local = jnp.where((local >= 0) & (local < BAND), local, -1.0).astype(BF16)
                for g in range(rows):
                    own_hot[t * BAND : (t + 1) * BAND, g * LANES : (g + 1) * LANES] = equal(band, local[g : g + 1])

    def owned_first():
        with jax.named_scope("owned"):
            settled(0)
            high, low = halves(out[0])
            split[:, :LANES] = high
            split[:, LANES:] = low
            both = dot(own_hot[...], split[...])
            own0[...] = both[:, :LANES] + both[:, LANES:]

    subs = range(SUBS)
    combine(0, 0)
    owned_places()
    combine(0, 1)
    combine(0, 2)
    s0 = combine_swap(0, 3)
    r0 = [reduce_start(0, s, s0[s]) for s in subs]
    combine(1, 0)
    combine(1, 1)
    g0 = [gather_start(0, 0, r0[0])]
    combine(1, 2)
    g0.append(gather_start(0, 1, r0[1]))
    s1 = combine_swap(1, 3)
    r1 = [reduce_start(1, s, s1[s]) for s in subs]
    f0 = [forward(0, s, g0[s]) for s in subs]
    g1 = [gather_start(1, 0, r1[0])]
    owned_first()
    g1.append(gather_start(1, 1, r1[1]))
    f1 = [forward(1, s, g1[s]) for s in subs]
    with jax.named_scope("last"):
        settled(1)
        for whole, sem in (
            (send.at[pl.ds(1, N_VOL - 1), pl.ds(0, CAP + 1)], p1s),
            (send.at[pl.ds(1, N_VOL - 1), pl.ds(FIRST, CAP)], p1s),
            (other, d2s),
            (parts, rss),
            (parts, ags),
            (out.at[:, pl.ds(0, HALF)], fws),
        ):
            remote(whole, whole, sem.at[0], d2r.at[0, 0], partner).wait_send()


def exchange(partial, pick, ids, tile_owner):
    vmem = pl.BlockSpec(memory_space=pltpu.VMEM)
    dma = pltpu.SemaphoreType.DMA
    return pl.pallas_call(
        exchange_kernel,
        out_shape=(
            jax.ShapeDtypeStruct((2, BLOCK_TILES, LANES), F32),
            jax.ShapeDtypeStruct((OWN_MAX, LANES), F32),
            jax.ShapeDtypeStruct((OWN_MAX, BLOCK_TILES), BF16),
        ),
        in_specs=[vmem] * 4,
        out_specs=(vmem,) * 3,
        scratch_shapes=[
            pltpu.VMEM((N_VOL, MSG, LANES), F32),
            pltpu.VMEM((N_VOL, MSG, LANES), F32),
            pltpu.VMEM((2, BLOCK_TILES, LANES), F32),
            pltpu.VMEM((2, SUBS, SUB, LANES), F32),
            pltpu.VMEM((2, SUBS, SIDE - 1, PIECE, LANES), F32),
            pltpu.VMEM((GROUP * CAP, 2 * LANES), BF16),
            pltpu.VMEM((BLOCK_TILES, N_VOL * CAP), BF16),
            pltpu.VMEM((BLOCK_TILES, 2 * LANES), BF16),
            dma((1,)), dma((2, N_VOL // GROUP)),
            dma((1,)), dma((2, SUBS)),
            dma((1,)), dma((2, SUBS)),
            dma((1,)), dma((2, SUBS, SIDE - 1)),
            dma((1,)), dma((2,)),
        ],
        compiler_params=pltpu.CompilerParams(
            collective_id=0, has_side_effects=True, vmem_limit_bytes=32 << 20
        ),
        name="exchange",
    )(partial, pick, ids, tile_owner)


def finish_kernel(map_ref, own0, own_hot, owned_h, shell_h, owned, rhs, sems):
    def put(source, target, n):
        c = pltpu.make_async_copy(source, target, sems.at[n])
        c.start()
        return c

    left, right = pl.ds(0, LANES), pl.ds(LANES, LANES)
    copies = [
        put(map_ref.at[1], shell_h.at[:, right], 0),
        put(map_ref.at[0], shell_h.at[:, left], 1),
        put(own0, owned_h.at[:, left], 2),
    ]
    high, low = halves(map_ref[1])
    rhs[:, :LANES] = high
    rhs[:, LANES:] = low
    both = dot(own_hot[...], rhs[...])
    owned[...] = both[:, :LANES] + both[:, LANES:]
    copies.append(put(owned, owned_h.at[:, right], 3))
    for c in copies:
        c.wait()


def finish(block_map, own0, own_hot):
    vmem = pl.BlockSpec(memory_space=pltpu.VMEM)
    return pl.pallas_call(
        finish_kernel,
        out_shape=(
            jax.ShapeDtypeStruct((OWN_MAX, 2 * LANES), F32),
            jax.ShapeDtypeStruct((BLOCK_TILES, 2 * LANES), F32),
        ),
        in_specs=[vmem] * 3,
        out_specs=(pl.BlockSpec(memory_space=pltpu.HBM),) * 2,
        scratch_shapes=[
            pltpu.VMEM((OWN_MAX, LANES), F32),
            pltpu.VMEM((BLOCK_TILES, 2 * LANES), BF16),
            pltpu.SemaphoreType.DMA((4,)),
        ],
        compiler_params=pltpu.CompilerParams(vmem_limit_bytes=16 << 20),
        name="finish",
    )(block_map, own0, own_hot)


def shards(kernel, pressure, velocity, entry_slot, slot_tile, tile_owner):
    square = (ENTRIES // LANES, LANES)
    partial, pick, ids = project(
        kernel,
        pressure.reshape(square),
        velocity.reshape(square),
        entry_slot.reshape(square),
        slot_tile.reshape(SLOTS // LANES, LANES),
    )
    block_map, own0, own_hot = exchange(partial, pick, ids, tile_owner.reshape(-1, LANES))
    return finish(block_map, own0, own_hot)


def solution(mesh):
    in_specs = (
        P(("vol", "pix"), None),
        P(("vol", "pix")),
        P(("vol", "pix")),
        P(("vol", "pix"), None),
        P(("vol", "pix"), None),
        P(),
    )
    out_specs = (P(("vol", "pix"), None), P("vol", None))
    return jax.shard_map(shards, mesh=mesh, in_specs=in_specs, out_specs=out_specs, check_vma=False)
```

```python
import functools

import jax
import jax.numpy as jnp
from jax import lax
from jax.experimental import pallas as pl
from jax.experimental.pallas import tpu as pltpu
from jax.sharding import PartitionSpec as P

MESH = pl.DeviceIdType.MESH
F32 = jnp.float32
BF16 = jnp.bfloat16

LANES = 128
ENTRIES = 16384
SLOTS = 1024
N_VOL = 16
SIDE = 4
BLOCK_TILES = 2048
CAP = 128
OWN_MAX = 512

STEP = 8192
SPAN = 256
WINDOW = 40
MSG = 2 * CAP + 8
FIRST = CAP + 8


def dot(a, b):
    return jnp.dot(a, b, preferred_element_type=F32)


def iota(shape, dim):
    return lax.broadcasted_iota(jnp.int32, shape, dim)


def halves(x):
    high = x.astype(BF16)
    return high, (x - high.astype(F32)).astype(BF16)


def equal(place, row):
    return jnp.where(place == row, jnp.ones((), BF16), jnp.zeros((), BF16))


def project_kernel(
    kernel_h, pressure_h, velocity_h, slot_h, tile_h, rhs_ref, pick_ref, ids_ref,
    weights, pressure, velocity, slot_v, tile_v, slot_s, acc, sems, chunk_sems,
):
    steps = ENTRIES // STEP
    rows = STEP // LANES
    small = [
        pltpu.make_async_copy(a, b, sems.at[n])
        for n, (a, b) in enumerate(
            (
                (tile_h, tile_v), (slot_h, slot_s), (slot_h, slot_v),
                (pressure_h, pressure), (velocity_h, velocity),
            )
        )
    ]
    for c in small:
        c.start()

    def chunk(g):
        span = pl.ds(pl.multiple_of(g * STEP, STEP), STEP)
        return pltpu.make_async_copy(kernel_h.at[span], weights.at[span], chunk_sems.at[g])

    for g in range(steps):
        chunk(g).start()
    acc[...] = jnp.zeros_like(acc)

    small[0].wait()
    tiles = tile_v[...]
    block = tiles // BLOCK_TILES
    within = tiles - block * BLOCK_TILES
    groups = SLOTS // LANES
    match = jnp.concatenate([(block == v).astype(F32) for v in range(N_VOL)], 0)
    r, c = iota((LANES, LANES), 0), iota((LANES, LANES), 1)
    before = (r < c).astype(F32).astype(BF16)
    above = ((c < r) & (c // groups == r // groups)).astype(F32).astype(BF16)
    ones = jnp.ones((LANES, LANES), BF16)
    packed = match.astype(BF16)
    rank = dot(packed, before) + dot(dot(above, packed).astype(BF16), ones)
    key = jnp.where(match > 0, rank, -1.0).astype(BF16)
    own = jnp.zeros((groups, LANES), F32)
    for v in range(N_VOL):
        own += match[v * groups : (v + 1) * groups] * rank[v * groups : (v + 1) * groups]
    place = iota((LANES, LANES), 0).astype(F32).astype(BF16)
    spread = jnp.concatenate([equal(place, own[g : g + 1].astype(BF16)) for g in range(groups)], 1)
    for v in range(N_VOL):
        for g in range(groups):
            row = v * groups + g
            pick_ref[v * CAP : (v + 1) * CAP, g * LANES : (g + 1) * LANES] = equal(place, key[row : row + 1])
    vols = iota((N_VOL, LANES), 0)
    upper, lower = (within // 64).astype(F32), (within % 64).astype(F32)
    table = []
    for values in (upper, lower, jnp.ones_like(upper)):
        table.append(
            jnp.concatenate(
                [jnp.where(vols == block[g : g + 1], values[g : g + 1], 0.0) for g in range(groups)], 1
            )
        )
    table = jnp.concatenate(table, 0).astype(BF16)
    found = lax.dot_general(table, spread, (((1,), (1,)), ((), ())), preferred_element_type=F32)
    ids_ref[...] = found[:N_VOL] * 64.0 + found[N_VOL : 2 * N_VOL] + found[2 * N_VOL :] - 1.0

    for n in (1, 2, 3, 4):
        small[n].wait()
    lines = iota((WINDOW, LANES), 0)
    per = SPAN // LANES

    @pl.loop(0, steps)
    def _(g):
        chunk(g).wait()
        top = pl.multiple_of(g * rows, rows)
        thermal = pressure[pl.ds(top, rows), :].astype(F32)
        kinetic = velocity[pl.ds(top, rows), :].astype(F32)
        slots = slot_v[pl.ds(top, rows), :]

        def products(i, base):
            up, low = [], []
            for h in range(per):
                n = i * per + h
                match = lines == slots[n : n + 1, :] - base
                up.append(jnp.where(match, thermal[n : n + 1, :], 0.0))
                low.append(jnp.where(match, kinetic[n : n + 1, :], 0.0))
            amplitudes = jnp.concatenate([jnp.concatenate(up, 1), jnp.concatenate(low, 1)], 0)
            span = pl.ds(pl.multiple_of(g * STEP + i * SPAN, SPAN), SPAN)
            return dot(amplitudes.astype(BF16), weights[span, :])

        def add(base, value):
            acc[0, pl.ds(base, WINDOW), :] += value[:WINDOW]
            acc[1, pl.ds(base, WINDOW), :] += value[WINDOW:]

        count = STEP // SPAN
        bases, lasts = [], []
        for i in range(count):
            bases.append(pl.multiple_of(slot_s[top + i * per, 0] & -8, 8))
            lasts.append(slot_s[top + i * per + per - 1, LANES - 1])
        values = [products(i, bases[i]) for i in range(count)]
        for i in range(count):
            add(bases[i], values[i])
        widest = lasts[0] - bases[0]
        for i in range(1, count):
            widest = jnp.maximum(widest, lasts[i] - bases[i])

        @pl.when(widest >= WINDOW)
        def _():
            for i in range(count):

                @pl.loop(1, (lasts[i] - bases[i]) // WINDOW + 1)
                def _(w, i=i):
                    base = pl.multiple_of(bases[i] + w * WINDOW, 8)
                    add(base, products(i, base))

    for ch in range(2):
        high, low = halves(acc[ch, :SLOTS, :])
        rhs_ref[:, 2 * ch * LANES : (2 * ch + 1) * LANES] = high
        rhs_ref[:, (2 * ch + 1) * LANES : (2 * ch + 2) * LANES] = low


def project(kernel, pressure, velocity, entry_slot, slot_tile):
    outs = (((SLOTS, 4 * LANES), BF16), ((N_VOL * CAP, SLOTS), BF16), ((N_VOL, LANES), F32))
    square = (ENTRIES // LANES, LANES)
    return pl.pallas_call(
        project_kernel,
        out_shape=tuple(jax.ShapeDtypeStruct(*o) for o in outs),
        in_specs=[pl.BlockSpec(memory_space=pltpu.HBM)] * 5,
        out_specs=tuple(pl.BlockSpec(memory_space=pltpu.VMEM) for o in outs),
        scratch_shapes=[
            pltpu.VMEM((ENTRIES, LANES), BF16),
            pltpu.VMEM(square, BF16),
            pltpu.VMEM(square, BF16),
            pltpu.VMEM(square, jnp.int32),
            pltpu.VMEM((SLOTS // LANES, LANES), jnp.int32),
            pltpu.SMEM(square, jnp.int32),
            pltpu.VMEM((2, SLOTS + WINDOW + 8, LANES), F32),
            pltpu.SemaphoreType.DMA((5,)),
            pltpu.SemaphoreType.DMA((ENTRIES // STEP,)),
        ],
        compiler_params=pltpu.CompilerParams(vmem_limit_bytes=16 << 20),
        name="project",
    )(*(pltpu.with_memory_space_constraint(a, pltpu.HBM) for a in (kernel, pressure, velocity, entry_slot, slot_tile)))


GROUPS = ((0, 5), (5, 4), (9, 4), (13, 3))
LARGEST = max(size for _, size in GROUPS)
SUBS = 2
HALF = BLOCK_TILES // 2
SUB = HALF // SUBS
PIECE = SUB // SIDE
TALL = 1024
BAND = 256
ORDER = (0, 4, 1, 12, 3, 8, 2, 5, 15, 13, 7, 9, 6, 11, 14, 10)
ROUND = 16


def group_of(n):
    return [start <= n < start + count for start, count in GROUPS].index(True)


def exchange_kernel(
    partial, pick, ids_ref, owner_ref, out, own0, own_hot, send, recv, acc, other, parts, rhs, hot, split,
    p1s, p1r, d2s, d2r, rss, rsr, ags, agr, fws, fwr,
):
    vol = lax.axis_index("vol")
    pix = lax.axis_index("pix")
    x, core = pix // 2, pix % 2
    y, z = vol // SIDE, vol % SIDE

    def vol_to(k):
        return lax.rem(y + k // SIDE, SIDE) * SIDE + lax.rem(z + k % SIDE, SIDE)

    def pix_to(k):
        return {"pix": lax.rem(x + k, SIDE) * 2 + core}

    partner = {"pix": x * 2 + 1 - core}
    peers = [{"vol": vol_to(k)} for k in range(1, N_VOL)] + [pix_to(k) for k in range(1, SIDE)] + [partner]
    barrier = pltpu.get_barrier_semaphore()
    for peer in peers:
        pl.semaphore_signal(barrier, inc=1, device_id=peer, device_id_type=MESH)

    def remote(src, dst, s, r, peer):
        return pltpu.make_async_remote_copy(
            src_ref=src, dst_ref=dst, send_sem=s, recv_sem=r, device_id=peer, device_id_type=MESH
        )

    def copy(src, dst, s, r, peer):
        c = remote(src, dst, s, r, peer)
        c.start()
        return c

    spans = ((0, CAP + 1), (FIRST, CAP))
    rows_of = (0, FIRST)
    def launch(ch, n):
        begin, size = spans[ch]
        copy(
            send.at[n, pl.ds(begin, size)],
            recv.at[n, pl.ds(begin, size)],
            p1s.at[0], p1r.at[ch, group_of(n)], {"vol": vol_to(ORDER[n])},
        )

    def arrived(ch, group):
        begin, size = spans[ch]
        start, count = GROUPS[group]
        low = max(start, 1)
        span = pl.ds(low, start + count - low)
        span = recv.at[span, pl.ds(begin, size)]
        remote(span, span, p1s.at[0], p1r.at[ch, group], partner).wait_recv()

    def batch(ch, ns):
        rows = []
        for n in ns:
            to = vol_to(ORDER[n])
            rows.append(pick[pl.ds(pl.multiple_of(to * CAP, CAP), CAP), :])
            if ch == 0:
                send[n, CAP:FIRST, :] = jnp.broadcast_to(ids_ref[pl.ds(to, 1), :], (8, LANES))
        both = dot(jnp.concatenate(rows, 0), partial[:, 2 * ch * LANES : 2 * (ch + 1) * LANES])
        total = both[:, :LANES] + both[:, LANES:]
        for m, n in enumerate(ns):
            send[n, rows_of[ch] : rows_of[ch] + CAP, :] = total[m * CAP : (m + 1) * CAP]

    todo = tuple(range(1, N_VOL)) + (0,)
    with jax.named_scope("messages"):
        for n in range(0, N_VOL, ROUND):
            batch(0, todo[n : n + ROUND])
        pl.semaphore_wait(barrier, len(peers))
        for n in range(1, N_VOL):
            launch(0, n)
        for n in range(0, N_VOL, ROUND):
            batch(1, todo[n : n + ROUND])

    def launch_second():
        for n in range(1, N_VOL):
            launch(1, n)

    band = iota((BAND, LANES), 0).astype(F32).astype(BF16)
    mine = core * HALF
    theirs = HALF - mine

    def load(ch, group):
        ids = []
        arrived(ch, group)
        if ch == 0 and group == 1:
            launch_second()
        for n in range(GROUPS[group][1]):
            k = GROUPS[group][0] + n
            source = recv if k else send
            ids.append(source[k, CAP : CAP + 1, :])
            high, low = halves(source[k, rows_of[ch] : rows_of[ch] + CAP, :])
            rhs[n * CAP : (n + 1) * CAP, :LANES] = high
            rhs[n * CAP : (n + 1) * CAP, LANES:] = low
        return ids

    def tiles(ch, group, ids, begin, count):
        start, count_in = GROUPS[group]
        columns = slice(start * CAP, (start + count_in) * CAP)

        def one(t):
            at = pl.multiple_of(begin + t * TALL, TALL)
            if ch == 0:
                for b in range(TALL // BAND):
                    low = pl.multiple_of(at + b * BAND, BAND)
                    pieces = []
                    for i in ids:
                        local = i - low.astype(F32)
                        local = jnp.where((local >= 0) & (local < BAND), local, -1.0)
                        pieces.append(equal(band, local.astype(BF16)))
                    hot[pl.ds(low, BAND), columns] = jnp.concatenate(pieces, 1)
            both = dot(hot[pl.ds(at, TALL), columns], rhs[: count_in * CAP, :])
            total = both[:, :LANES] + both[:, LANES:]
            if group:
                total += acc[ch, pl.ds(at, TALL), :]
            acc[ch, pl.ds(at, TALL), :] = total

        if count == 1:
            one(0)
        else:
            pl.loop(0, count)(one)

    def combine(ch, group):
        with jax.named_scope(f"load{ch}{group}"):
            ids = load(ch, group)
        with jax.named_scope(f"combine{ch}{group}"):
            tiles(ch, group, ids, jnp.int32(0), BLOCK_TILES // TALL)

    def combine_swap(ch, group):
        with jax.named_scope(f"load{ch}{group}"):
            ids = load(ch, group)
        copies = []
        with jax.named_scope(f"combine{ch}{group}"):
            tiles(ch, group, ids, theirs, HALF // TALL)
            for s in range(SUBS):
                at = pl.multiple_of(theirs + s * SUB, SUB)
                copies.append(
                    copy(acc.at[ch, pl.ds(at, SUB)], other.at[ch, s], d2s.at[0], d2r.at[ch, s], partner)
                )
            tiles(ch, group, ids, mine, HALF // TALL)
        return copies

    def reduce_start(ch, s, swapped):
        with jax.named_scope(f"reduce{ch}{s}"):
            swapped.wait_recv()
            acc[ch, pl.ds(pl.multiple_of(mine + s * SUB, SUB), SUB), :] += other[ch, s]
            copies = []
            for k in (2, 1, 3):
                at = pl.multiple_of(mine + s * SUB + lax.rem(x + k, SIDE) * PIECE, PIECE)
                copies.append(
                    copy(
                        acc.at[ch, pl.ds(at, PIECE)], parts.at[ch, s, k - 1],
                        rss.at[0], rsr.at[ch, s], pix_to(k),
                    )
                )
        return copies

    def gather_start(ch, s, copies):
        with jax.named_scope(f"gather{ch}{s}"):
            here = pl.multiple_of(mine + s * SUB + x * PIECE, PIECE)
            remote(parts.at[ch, s], parts.at[ch, s], rss.at[0], rsr.at[ch, s], partner).wait_recv()
            total = acc[ch, pl.ds(here, PIECE), :]
            for k in range(1, SIDE):
                total += parts[ch, s, k - 1]
            out[ch, pl.ds(here, PIECE), :] = total
            block = out.at[ch, pl.ds(here, PIECE)]
            gathers = [
                (k, copy(block, block, ags.at[0], agr.at[ch, s, k - 1], pix_to(k))) for k in (2, 1, 3)
            ]
        return gathers, [copy(block, block, fws.at[0], fwr.at[ch], partner)]

    def forward(ch, s, started_gathers):
        gathers, sent = started_gathers
        with jax.named_scope(f"forward{ch}{s}"):
            for k, c in (gathers[1], gathers[2], gathers[0]):
                c.wait_recv()
                at = pl.multiple_of(mine + s * SUB + lax.rem(x - k + SIDE, SIDE) * PIECE, PIECE)
                block = out.at[ch, pl.ds(at, PIECE)]
                copy(block, block, fws.at[0], fwr.at[ch], partner)
        return sent

    def settled(ch):
        block = out.at[ch, pl.ds(pl.multiple_of(theirs, HALF), HALF)]
        remote(block, block, fws.at[0], fwr.at[ch], partner).wait_recv()

    def owned_places():
        with jax.named_scope("places"):
            rows = BLOCK_TILES // LANES
            owner = owner_ref[pl.ds(pl.multiple_of(vol * rows, rows), rows), :]
            match = (owner == pix).astype(F32)
            packed = match.astype(BF16)
            before = (iota((LANES, LANES), 0) < iota((LANES, LANES), 1)).astype(F32).astype(BF16)
            above = (iota((rows, rows), 1) < iota((rows, rows), 0)).astype(F32).astype(BF16)
            ones = jnp.ones((LANES, LANES), BF16)
            rank = dot(packed, before) + dot(dot(above, packed).astype(BF16), ones)
            key = jnp.where(match > 0, rank, -1.0)
            for t in range(OWN_MAX // BAND):
                local = key - t * BAND
                local = jnp.where((local >= 0) & (local < BAND), local, -1.0).astype(BF16)
                for g in range(rows):
                    own_hot[t * BAND : (t + 1) * BAND, g * LANES : (g + 1) * LANES] = equal(band, local[g : g + 1])

    def owned_first():
        with jax.named_scope("owned"):
            settled(0)
            high, low = halves(out[0])
            split[:, :LANES] = high
            split[:, LANES:] = low
            both = dot(own_hot[...], split[...])
            own0[...] = both[:, :LANES] + both[:, LANES:]

    subs = range(SUBS)
    combine(0, 0)
    owned_places()
    combine(0, 1)
    combine(0, 2)
    s0 = combine_swap(0, 3)
    r0 = [reduce_start(0, s, s0[s]) for s in subs]
    combine(1, 0)
    combine(1, 1)
    g0 = [gather_start(0, 0, r0[0])]
    combine(1, 2)
    g0.append(gather_start(0, 1, r0[1]))
    s1 = combine_swap(1, 3)
    r1 = [reduce_start(1, s, s1[s]) for s in subs]
    f0 = [forward(0, s, g0[s]) for s in subs]
    g1 = [gather_start(1, 0, r1[0])]
    owned_first()
    g1.append(gather_start(1, 1, r1[1]))
    f1 = [forward(1, s, g1[s]) for s in subs]
    with jax.named_scope("last"):
        settled(1)
        for whole, sem in (
            (send.at[pl.ds(1, N_VOL - 1), pl.ds(0, CAP + 1)], p1s),
            (send.at[pl.ds(1, N_VOL - 1), pl.ds(FIRST, CAP)], p1s),
            (other, d2s),
            (parts, rss),
            (parts, ags),
            (out.at[:, pl.ds(0, HALF)], fws),
        ):
            remote(whole, whole, sem.at[0], d2r.at[0, 0], partner).wait_send()


def exchange(partial, pick, ids, tile_owner):
    vmem = pl.BlockSpec(memory_space=pltpu.VMEM)
    dma = pltpu.SemaphoreType.DMA
    return pl.pallas_call(
        exchange_kernel,
        out_shape=(
            jax.ShapeDtypeStruct((2, BLOCK_TILES, LANES), F32),
            jax.ShapeDtypeStruct((OWN_MAX, LANES), F32),
            jax.ShapeDtypeStruct((OWN_MAX, BLOCK_TILES), BF16),
        ),
        in_specs=[vmem] * 4,
        out_specs=(vmem,) * 3,
        scratch_shapes=[
            pltpu.VMEM((N_VOL, MSG, LANES), F32),
            pltpu.VMEM((N_VOL, MSG, LANES), F32),
            pltpu.VMEM((2, BLOCK_TILES, LANES), F32),
            pltpu.VMEM((2, SUBS, SUB, LANES), F32),
            pltpu.VMEM((2, SUBS, SIDE - 1, PIECE, LANES), F32),
            pltpu.VMEM((LARGEST * CAP, 2 * LANES), BF16),
            pltpu.VMEM((BLOCK_TILES, N_VOL * CAP), BF16),
            pltpu.VMEM((BLOCK_TILES, 2 * LANES), BF16),
            dma((1,)), dma((2, len(GROUPS))),
            dma((1,)), dma((2, SUBS)),
            dma((1,)), dma((2, SUBS)),
            dma((1,)), dma((2, SUBS, SIDE - 1)),
            dma((1,)), dma((2,)),
        ],
        compiler_params=pltpu.CompilerParams(
            collective_id=0, has_side_effects=True, vmem_limit_bytes=32 << 20
        ),
        name="exchange",
    )(partial, pick, ids, tile_owner)


def finish_kernel(map_ref, own0, own_hot, owned_h, shell_h, owned, rhs, sems):
    def put(source, target, n):
        c = pltpu.make_async_copy(source, target, sems.at[n])
        c.start()
        return c

    left, right = pl.ds(0, LANES), pl.ds(LANES, LANES)
    copies = [
        put(map_ref.at[1], shell_h.at[:, right], 0),
        put(map_ref.at[0], shell_h.at[:, left], 1),
        put(own0, owned_h.at[:, left], 2),
    ]
    high, low = halves(map_ref[1])
    rhs[:, :LANES] = high
    rhs[:, LANES:] = low
    both = dot(own_hot[...], rhs[...])
    owned[...] = both[:, :LANES] + both[:, LANES:]
    copies.append(put(owned, owned_h.at[:, right], 3))
    for c in copies:
        c.wait()


def finish(block_map, own0, own_hot):
    vmem = pl.BlockSpec(memory_space=pltpu.VMEM)
    return pl.pallas_call(
        finish_kernel,
        out_shape=(
            jax.ShapeDtypeStruct((OWN_MAX, 2 * LANES), F32),
            jax.ShapeDtypeStruct((BLOCK_TILES, 2 * LANES), F32),
        ),
        in_specs=[vmem] * 3,
        out_specs=(pl.BlockSpec(memory_space=pltpu.HBM),) * 2,
        scratch_shapes=[
            pltpu.VMEM((OWN_MAX, LANES), F32),
            pltpu.VMEM((BLOCK_TILES, 2 * LANES), BF16),
            pltpu.SemaphoreType.DMA((4,)),
        ],
        compiler_params=pltpu.CompilerParams(vmem_limit_bytes=16 << 20),
        name="finish",
    )(block_map, own0, own_hot)


def shards(kernel, pressure, velocity, entry_slot, slot_tile, tile_owner):
    square = (ENTRIES // LANES, LANES)
    partial, pick, ids = project(
        kernel,
        pressure.reshape(square),
        velocity.reshape(square),
        entry_slot.reshape(square),
        slot_tile.reshape(SLOTS // LANES, LANES),
    )
    block_map, own0, own_hot = exchange(partial, pick, ids, tile_owner.reshape(-1, LANES))
    return finish(block_map, own0, own_hot)


def solution(mesh):
    in_specs = (
        P(("vol", "pix"), None),
        P(("vol", "pix")),
        P(("vol", "pix")),
        P(("vol", "pix"), None),
        P(("vol", "pix"), None),
        P(),
    )
    out_specs = (P(("vol", "pix"), None), P("vol", None))
    return jax.shard_map(shards, mesh=mesh, in_specs=in_specs, out_specs=out_specs, check_vma=False)
```
